32 devices in a mesh: rows: 8 (over z, x), feat: 4 (over y, core).
Axes of the slice: x: 2, y: 2, z: 4, core: 2. Of those that a mesh axis runs over, the one named last changes fastest.
Arguments:
- tile_values: bfloat16 [2048, 256, 128], P('rows', 'feat'), may hold values from -6 to 6
- tile_blocks: int32 [2048, 256], P('rows', 'feat'), may hold values from 0 to 2047
- tile_counts: int32 [2048, 4], P('rows', 'feat'), may hold values from 1 to 64, as said below
- labels: int32 [2048], P('rows'), may hold values 0 or 1
- owner_rank: int32 [2048], P('rows'), may hold values from 0 to 7, as said below
- weights: float32 [8192, 128], P(('feat', 'rows')), may hold values from -0.09375 to 0.09375
Outputs:
- owned_margins: float32 [2048], P('rows')
- gradient: float32 [8192, 128], P(('feat', 'rows'))
- loss: float32 [], replicated
The draws below stay inside these ranges and needn't reach their ends.
Inputs may be any that keep to these rules, and one draw needn't show every extreme that they name: `owner_rank`: within each aligned block of 256 examples, every owner is named by exactly 32 examples. `tile_counts`: in every aligned block of 256 examples, each shard's column holds at least one example with exactly 64 used slots.
All inputs are finite; a program needn't handle non-finite values. No bound on the sum of `labels` on one device may be relied on, other than what follows from the above.
Results may differ from the reference program's by a relative error of at most 0.003.
Values may be sent and summed in bfloat16 or wider, within the bound.
A program may use at most 64 MiB of HBM per device.

```python
import jax
import jax.numpy as jnp
from jax import lax

TILE = 128
EX_DEV = 256
TPAD = 64
EXAMPLES = 2048
SLOTS = 256
NBLK = 8192
BLK_SHARD = 2048
PER_PEER = 32
N_ROWS = 8
N_FEAT = 4


def draw_tile_counts(key, part):
    device_count = EXAMPLES // EX_DEV
    shard_count = SLOTS // TPAD
    key_shift = jax.random.fold_in(key, 11)
    key_value = jax.random.fold_in(key, 12)
    key_full = jax.random.fold_in(key, 13)
    device_of = jnp.arange(EXAMPLES, dtype=jnp.int32) // EX_DEV
    spread = max(device_count - 1, 1)
    ceiling = TPAD * (spread + 2 * device_of) // (3 * spread)
    ceiling = jnp.maximum(ceiling, 1)
    shifts = jax.random.randint(key_shift, (EXAMPLES, shard_count), 0, 4)
    divisor = jnp.left_shift(jnp.ones_like(shifts), shifts)
    upper = jnp.maximum(ceiling[:, None] // divisor, 1)
    raw_value = jax.random.randint(key_value, (EXAMPLES, shard_count), 0, 1048576)
    drawn = raw_value % upper + 1
    chosen = jax.random.randint(key_full, (device_count, shard_count), 0, EX_DEV)
    local_index = jnp.arange(EXAMPLES, dtype=jnp.int32) % EX_DEV
    marked = local_index[:, None] == jnp.repeat(chosen, EX_DEV, axis=0)
    return jnp.where(marked, TPAD, drawn).astype(jnp.int32)


def one_block_owner(block_key):
    return jax.random.permutation(block_key, EX_DEV)


def draw_owner_rank(key, part):
    device_count = EXAMPLES // EX_DEV
    block_keys = jax.random.split(jax.random.fold_in(key, 21), device_count)
    shuffled = jax.vmap(one_block_owner)(block_keys)
    return (shuffled // PER_PEER).reshape(EXAMPLES).astype(jnp.int32)


def set_ends(values, key, smallest, high):
    extent = values.shape
    place = [jax.random.randint(jax.random.fold_in(key, axis), (), 0, extent[axis]) for axis in range(len(extent))]
    values = values.at[tuple(place)].set(smallest)
    longest = extent.index(max(extent))
    place[longest] = (place[longest] + 1) % extent[longest]
    return values.at[tuple(place)].set(high)


def levels(rng, dims, pieces, smallest, largest):
    def one(dim, blocks):
        draws = jax.random.uniform(jax.random.fold_in(jax.random.fold_in(rng, 6), dim), (blocks,), jnp.float32, smallest / len(pieces), largest / len(pieces))
        return jnp.repeat(jnp.exp(draws), dims[dim] // blocks).reshape((-1,) + (1,) * (len(dims) - dim - 1))

    factor_of = one(*pieces[0])
    for cut in pieces[1:]:
        factor_of = factor_of * one(*cut)
    return factor_of


def bell_draw(stream_key, dims, width, bound, cuts=(), held_as=jnp.bfloat16):
    loudness = levels(stream_key, dims, cuts, -0.22, 0.18) if cuts else 1.0
    array = jax.random.normal(stream_key, dims, jnp.float32) * width * loudness
    return jnp.minimum(jnp.maximum(array, -bound), bound).astype(held_as)


def setup_inputs(seed: int = 0) -> dict:
    splits = jax.random.split(jax.random.key(seed), 7)
    return {
        "tile_values": bell_draw(splits[0], (EXAMPLES, SLOTS, TILE), 1.0, 6.0, ((0, 8), (1, 4))),
        "tile_blocks": set_ends(jax.random.randint(splits[1], (EXAMPLES, SLOTS), 0, BLK_SHARD), jax.random.fold_in(splits[1], 1), 0, BLK_SHARD - 1).astype(jnp.int32),
        "tile_counts": draw_tile_counts(jax.random.fold_in(splits[6], 71), 0),
        "labels": set_ends((jax.random.randint(splits[3], (EXAMPLES,), 0, 2) < 1).astype(jnp.int32), jax.random.fold_in(splits[3], 1), 0, 1),
        "owner_rank": draw_owner_rank(jax.random.fold_in(splits[6], 71), 0),
        "weights": bell_draw(splits[5], (NBLK, TILE), (TPAD * TPAD) ** -0.5, 0.09375, ((0, 32),), jnp.float32),
    }


def reference(tile_values, tile_blocks, tile_counts, labels, owner_rank, weights):
    w_half = weights.astype(jnp.bfloat16)
    slot_index = jnp.arange(TPAD, dtype=jnp.int32)

    def shard_pieces(shard_index):
        values = lax.dynamic_slice_in_dim(tile_values, shard_index * TPAD, TPAD, 1)
        block_ids = lax.dynamic_slice_in_dim(tile_blocks, shard_index * TPAD, TPAD, 1)
        used = lax.dynamic_slice_in_dim(tile_counts, shard_index, 1, 1)
        live_slot = slot_index[None, :] < used
        return values, block_ids, live_slot

    def shard_margin(shard_index):
        values, block_ids, live_slot = shard_pieces(shard_index)
        weight_table = lax.dynamic_slice_in_dim(w_half, shard_index * BLK_SHARD, BLK_SHARD, 0)
        picked = weight_table[block_ids]
        products = jnp.sum(values.astype(jnp.float32) * picked.astype(jnp.float32), axis=2)
        return jnp.sum(jnp.where(live_slot, products, jnp.float32(0.0)), axis=1)

    shard_index_all = jnp.arange(N_FEAT, dtype=jnp.int32)
    partials = lax.map(shard_margin, shard_index_all)
    margin = jnp.sum(partials, axis=0)
    label_float = labels.astype(jnp.float32)
    residual = jax.nn.sigmoid(margin) - label_float
    loss = jnp.sum(jax.nn.softplus(margin) - label_float * margin) / EXAMPLES
    resid_half = residual.astype(jnp.bfloat16)

    def shard_gradient(shard_index):
        values, block_ids, live_slot = shard_pieces(shard_index)
        coefficient = jnp.where(live_slot, resid_half[:, None], jnp.zeros((), jnp.bfloat16))
        weighted = values.astype(jnp.float32) * coefficient.astype(jnp.float32)[:, :, None]
        return jax.ops.segment_sum(weighted.reshape(-1, TILE), block_ids.reshape(-1), num_segments=BLK_SHARD)

    gradient = lax.map(shard_gradient, shard_index_all).reshape(NBLK, TILE)
    owners = owner_rank.reshape(N_ROWS, EX_DEV)
    send_order = jnp.argsort(owners, axis=1, stable=True).astype(jnp.int32)
    source = send_order + (jnp.arange(N_ROWS, dtype=jnp.int32) * EX_DEV)[:, None]
    source = jnp.transpose(source.reshape(N_ROWS, N_ROWS, PER_PEER), (1, 0, 2)).reshape(EXAMPLES)
    owned_margins = margin[source]
    return owned_margins, gradient, loss
```

```python
import functools

import jax
import jax.numpy as jnp
from jax import lax
from jax.experimental import pallas as pl
from jax.experimental.pallas import tpu as pltpu
from jax.sharding import PartitionSpec as P

MESH = pl.DeviceIdType.MESH
LANES = 128
GRAIN = 16
GROUP = 32
GRANT = 24 * 1024 * 1024
COST = pl.CostEstimate(flops=0, bytes_accessed=24 * 1024 * 1024, transcendentals=0)
NT = (((1,), (1,)), ((), ()))
NN = (((1,), (0,)), ((), ()))
VM = pl.BlockSpec(memory_space=pltpu.VMEM)
SM = pl.BlockSpec(memory_space=pltpu.SMEM)
ANY = pl.BlockSpec(memory_space=pltpu.HBM)
WIDE = GROUP * GRAIN
PER = LANES // GRAIN


def seat(n):
    me = lax.axis_index("rows")
    side = lax.rem(me, 2)
    partner = me + 1 - 2 * side
    column = [lax.rem(me + 2 * k, n) for k in range(n // 2)]
    source = [lax.rem(me + n - 2 * k, n) for k in range(n // 2)]
    return me, partner, column, source


def call_out(axis, peers):
    barrier = pltpu.get_barrier_semaphore()
    for peer in peers:
        pl.semaphore_signal(barrier, inc=1, device_id={axis: peer}, device_id_type=MESH)
    return lambda: pl.semaphore_wait(barrier, len(peers))


def send_to(axis, peer, source, target, send, recv):
    copy = pltpu.make_async_remote_copy(
        src_ref=source,
        dst_ref=target,
        send_sem=send,
        recv_sem=recv,
        device_id={axis: peer},
        device_id_type=MESH,
    )
    copy.start()
    return copy


def lane_group():
    return lax.broadcasted_iota(jnp.int32, (1, LANES), 1) // GRAIN


def gather_kernel(
    n, w_hbm, ids_hbm, used_hbm, owner_hbm, vals_hbm,
    table_ref, x2_ref, hi_ref, lists_ref, rank_ref, owner_ref,
    w_buf, half, ids, used, own, vals, idt, lists, glist,
    send, recv, xsend, xrecv, here,
):
    local = [
        pltpu.make_async_copy(w_hbm, w_buf, here.at[0]),
        pltpu.make_async_copy(used_hbm, used, here.at[1]),
        pltpu.make_async_copy(ids_hbm, ids, here.at[2]),
        pltpu.make_async_copy(owner_hbm, own, here.at[3]),
        pltpu.make_async_copy(vals_hbm, vals, here.at[4]),
    ]
    for copy in local:
        copy.start()
    me, partner, column, source = seat(n)
    deep = n // 2
    rows = w_buf.shape[0]
    slots, ex = ids.shape
    grains = slots // GRAIN
    joined = call_out("rows", [partner] + column[1:])
    local[0].wait()
    half[...] = w_buf[...].astype(jnp.bfloat16)
    joined()
    across = [send_to("rows", partner, half, table_ref.at[me], xsend.at[0], xrecv.at[0])]
    along = [
        send_to("rows", column[k], half, table_ref.at[me], send.at[k - 1], recv.at[k - 1])
        for k in range(1, deep)
    ]
    table_ref[me] = w_buf[...].astype(jnp.bfloat16)

    f32 = jnp.float32
    local[1].wait()
    count = (used[...] + (GRAIN - 1)) // GRAIN
    sizes = jnp.broadcast_to(count, (LANES, ex)).T
    down = lax.broadcasted_iota(jnp.int32, (ex, LANES), 0)
    ends = sizes
    step = 1
    while step < ex:
        ends = ends + jnp.where(down >= step, pltpu.roll(ends, step, 0), 0)
        step *= 2
    lane = lax.broadcasted_iota(jnp.int32, (1, LANES), 1)
    span = ex * grains // LANES
    for b in range(span):
        place = lane + b * LANES
        past = ends <= place
        which = jnp.sum(jnp.where(past, 1, 0), axis=0, keepdims=True)
        begin = jnp.sum(jnp.where(past, sizes, 0), axis=0, keepdims=True)
        live = which < ex
        q = place - begin
        lists[b : b + 1, :] = jnp.clip(jnp.where(live, which * grains + q, 0), 0, grains * ex - 1)
        lists[span + b : span + b + 1, :] = jnp.clip(jnp.where(live, which + q * ex, grains * ex), 0, grains * ex)
    turns = (ends[ex - 8 : ex, :] + (GROUP - 1)) // GROUP
    lists[2 * span :, :] = jnp.broadcast_to(turns[7:8, :], (8, LANES))
    to_list = pltpu.make_async_copy(lists, glist, here.at[5])
    to_list.start()
    to_next = pltpu.make_async_copy(lists, lists_ref, here.at[6])
    to_next.start()

    local[2].wait()
    live = lax.broadcasted_iota(jnp.int32, (slots, ex), 0) < used[...]
    shifted = jnp.where(live, ids[...] + 1, 0)
    if slots < LANES:
        shifted = jnp.concatenate([shifted, jnp.zeros((LANES - slots, ex), jnp.int32)], axis=0)
    shifted = shifted.T
    spot = lax.broadcasted_iota(jnp.int32, (ex, LANES), 1) // GRAIN
    for q in range(grains):
        piece = jnp.where(spot == q, shifted, 0)
        step = GRAIN
        while step < LANES:
            piece = piece + pltpu.roll(piece, step, 1)
            step *= 2
        idt[q * ex : (q + 1) * ex, :] = piece - 1
    idt[grains * ex :, :] = jnp.full((8, LANES), -1, jnp.int32)

    local[3].wait()
    owner = own[...].astype(f32)
    square = jnp.broadcast_to(owner, (ex, ex))
    earlier = lax.broadcasted_iota(jnp.int32, (ex, ex), 0) < lax.broadcasted_iota(jnp.int32, (ex, ex), 1)
    same = jnp.where(jnp.logical_and(square.T == square, earlier), 1.0, 0.0)
    shift = lax.rem(me * (ex // n), LANES).astype(f32)
    rank = jnp.sum(same, axis=0, keepdims=True) + shift
    spots = lax.broadcasted_iota(jnp.int32, (LANES, ex), 0).astype(f32)
    rank_ref[...] = jnp.where(spots == rank, 1.0, 0.0)
    owner_ref[...] = jnp.broadcast_to(owner, owner_ref.shape)

    to_list.wait()
    to_next.wait()
    local[4].wait()
    group = lane_group()
    tall = x2_ref.shape[1] // 2

    def prepare(t, carry):
        row = t * GROUP // LANES
        col = lax.rem(t * GROUP, LANES)
        values = jnp.concatenate([vals[glist[row, col + i]] for i in range(GROUP)], axis=0)
        parts = []
        for h in range(GROUP // PER):
            line = idt[pl.ds(glist[span + row, col + h * PER], 1), :]
            for i in range(1, PER):
                line = jnp.where(group == i, idt[pl.ds(glist[span + row, col + h * PER + i], 1), :], line)
            parts.append(line)
        id_row = jnp.concatenate(parts, axis=1)
        chunk = id_row // rows
        odd = lax.rem(chunk, 2)
        high = jnp.where(id_row < 0, -1, (chunk // 2) * rows + lax.rem(id_row, rows))
        hi_ref[t] = high
        odd = jnp.broadcast_to(odd.astype(f32), (16, WIDE))
        odd_half = jnp.concatenate([odd.astype(jnp.bfloat16)] * (tall // 16), axis=0)
        even_half = jnp.concatenate([(1.0 - odd).astype(jnp.bfloat16)] * (tall // 16), axis=0)
        flipped = values.T
        x2_ref[t, 0:tall, :] = flipped * even_half
        x2_ref[t, tall:, :] = flipped * odd_half
        return carry

    total = x2_ref.shape[0]
    for k in range(deep):
        if k > 0:
            along[k - 1].wait_recv()
            block = table_ref.at[source[k]]
            across.append(send_to("rows", partner, block, block, xsend.at[k], xrecv.at[k]))
        lax.fori_loop(total * k // deep, total * (k + 1) // deep, prepare, jnp.int32(0))
    for copy in along:
        copy.wait_send()
    for copy in across:
        copy.wait()


def margin_kernel(lists, table_ref, x2_ref, hi_ref, partial_ref, terms):
    n, rows, _ = table_ref.shape
    ex = partial_ref.shape[1]
    grains = terms.shape[0] // ex
    span = ex * grains // LANES
    terms[...] = jnp.zeros_like(terms)
    group = lane_group()

    def turn(t, carry):
        x2 = x2_ref[t]
        offset = jnp.broadcast_to(hi_ref[t], (8, WIDE)) - lax.broadcasted_iota(jnp.int32, (8, WIDE), 0)
        found = jnp.zeros((8, WIDE), jnp.float32)
        for k in range(n // 2):
            pair = jnp.concatenate([table_ref[2 * k], table_ref[2 * k + 1]], axis=1)
            scores = lax.dot_general(pair, x2, NN, preferred_element_type=jnp.float32)
            for i in range(rows // 8):
                found = jnp.where(offset == k * rows + i * 8, scores[i * 8 : i * 8 + 8, :], found)
        term = jnp.sum(found, axis=0, keepdims=True)
        row = t * GROUP // LANES
        col = lax.rem(t * GROUP, LANES)
        for i in range(GROUP):
            h = i // PER
            mine = jnp.where(group == i % PER, term[:, h * LANES : (h + 1) * LANES], 0.0)
            terms[pl.ds(lists[span + row, col + i], 1), :] = mine
        return carry

    lax.fori_loop(0, lists[2 * span, 0], turn, jnp.int32(0))
    spread = terms[0:ex, :]
    for q in range(1, grains):
        spread = spread + terms[q * ex : (q + 1) * ex, :]
    partial_ref[...] = jnp.broadcast_to(jnp.sum(spread.T, axis=0, keepdims=True), partial_ref.shape)


def residual_kernel(n, partial_ref, labels_ref, margin_ref, resid_ref, loss_ref, held, send, recv):
    me = lax.axis_index("feat")
    peers = [lax.rem(me + k, n) for k in range(1, n)]
    call_out("feat", peers)()
    copies = [
        send_to("feat", peer, partial_ref, held.at[me], send.at[k], recv.at[k])
        for k, peer in enumerate(peers)
    ]
    held[me] = partial_ref[...]
    for copy in copies:
        copy.wait()
    margin = held[0]
    for k in range(1, n):
        margin = margin + held[k]
    label = labels_ref[...].astype(jnp.float32)
    residual = 1.0 / (1.0 + jnp.exp(-margin)) - label
    margin_ref[...] = margin
    resid_ref[...] = residual.astype(jnp.bfloat16).astype(jnp.float32)[0:1, :]
    term = jnp.maximum(margin, 0.0) + jnp.log1p(jnp.exp(-jnp.abs(margin))) - label * margin
    total = term[:, 0:LANES]
    for h in range(1, term.shape[1] // LANES):
        total = total + term[:, h * LANES : (h + 1) * LANES]
    loss_ref[...] = total


def gradient_kernel(grains, lists, resid, x2_ref, hi_ref, out_ref, total):
    total[...] = jnp.zeros_like(total)
    n, rows, width = out_ref.shape
    span = resid.shape[1] * grains // LANES
    group = lane_group()

    def turn(t, carry):
        x2 = x2_ref[t]
        offset = jnp.broadcast_to(hi_ref[t], (8, WIDE)) - lax.broadcasted_iota(jnp.int32, (8, WIDE), 0)
        row_at = t * GROUP // LANES
        col = lax.rem(t * GROUP, LANES)
        parts = []
        for h in range(GROUP // PER):
            row = jnp.zeros((1, LANES), jnp.float32)
            for i in range(PER):
                row = jnp.where(group == i, resid[0, lists[row_at, col + h * PER + i] // grains], row)
            parts.append(row)
        factor = jnp.broadcast_to(jnp.concatenate(parts, axis=1), (8, WIDE))
        for k in range(n // 2):
            spread = jnp.concatenate(
                [jnp.where(offset == k * rows + i * 8, factor, 0.0) for i in range(rows // 8)], axis=0
            ).astype(jnp.bfloat16)
            total[k * rows : (k + 1) * rows, :] += lax.dot_general(
                spread, x2, NT, preferred_element_type=jnp.float32
            )
        return carry

    lax.fori_loop(0, lists[2 * span, 0], turn, jnp.int32(0))
    for k in range(n // 2):
        out_ref[2 * k] = total[k * rows : (k + 1) * rows, 0:width].astype(jnp.bfloat16)
        out_ref[2 * k + 1] = total[k * rows : (k + 1) * rows, width:].astype(jnp.bfloat16)


def scatter_kernel(
    n, grad_ref, margin_ref, owner_ref, rank_ref, loss_ref,
    sum_ref, notes_ref, notes, crossed, paired, held, send, recv, xsend, xrecv, nsend, nrecv,
):
    ex = margin_ref.shape[1]
    me, partner, column, source = seat(n)
    side = me - partner
    deep = n // 2
    others = [lax.rem(me + k, n) for k in range(1, n)]
    joined = call_out("rows", others)
    which = lax.broadcasted_iota(jnp.int32, (n, ex), 0).astype(jnp.float32)
    by_owner = jnp.where(which == owner_ref[0:1, :], margin_ref[0:1, :], 0.0)
    ordered = lax.dot_general(
        by_owner, rank_ref[...], NT, precision=lax.Precision.HIGHEST, preferred_element_type=jnp.float32
    )
    sub = lax.broadcasted_iota(jnp.int32, (8, LANES), 0)
    for d in range(n):
        notes[d] = jnp.where(sub == 0, ordered[d : d + 1, :], loss_ref[...])
    joined()
    order = list(range(1, deep)) + [0]
    across = {
        k: send_to("rows", partner, grad_ref.at[column[k] - side], crossed.at[k], xsend.at[k], xrecv.at[k])
        for k in order
    }
    told = [
        send_to("rows", peer, notes.at[peer], notes_ref.at[me], nsend.at[k], nrecv.at[k])
        for k, peer in enumerate(others)
    ]
    notes_ref[me] = notes[me]
    along = []
    for k in range(1, deep):
        across[k].wait_recv()
        pair = grad_ref[column[k]].astype(jnp.float32) + crossed[k].astype(jnp.float32)
        paired[k - 1] = pair.astype(jnp.bfloat16)
        along.append(
            send_to("rows", column[k], paired.at[k - 1], held.at[k - 1], send.at[k - 1], recv.at[k - 1])
        )
    across[0].wait_recv()
    total = grad_ref[me].astype(jnp.float32) + crossed[0].astype(jnp.float32)
    for k in range(1, deep):
        along[k - 1].wait_recv()
        total = total + held[k - 1].astype(jnp.float32)
    sum_ref[...] = total
    for k in order:
        across[k].wait_send()
    for copy in along:
        copy.wait_send()
    for copy in told:
        copy.wait()


def finish_kernel(sum_ref, notes_ref, owned_ref, grad_ref, loss_ref):
    n = notes_ref.shape[0]
    ex = owned_ref.shape[1]
    grad_ref[...] = sum_ref[...]
    for h in range(ex // LANES):
        row = jnp.zeros((1, LANES), jnp.float32)
        for d in range(n):
            if d * (ex // n) // LANES == h:
                row = row + notes_ref[d, 0:1, :]
        owned_ref[:, h * LANES : (h + 1) * LANES] = row
    loss = jnp.zeros((1, LANES), jnp.float32)
    for d in range(n):
        loss = loss + notes_ref[d, 1:2, :]
    loss_ref[0, 0] = jnp.sum(loss) * (1.0 / (ex * n))


def on_device(n, nf, tile_values, tile_blocks, tile_counts, labels, owner_rank, weights):
    ex, slots, width = tile_values.shape
    grains = slots // GRAIN
    rows = weights.shape[0]
    deep = n // 2
    turns = ex * grains // GROUP
    span = ex * grains // LANES
    f32, i32, bf16 = jnp.float32, jnp.int32, jnp.bfloat16
    shape = jax.ShapeDtypeStruct
    dma = pltpu.SemaphoreType.DMA
    vals = tile_values.reshape(ex * grains, GRAIN, width)

    table, x2, high, lists, rank, owner = pl.pallas_call(
        functools.partial(gather_kernel, n),
        out_shape=(
            shape((n, rows, width), bf16),
            shape((turns, 2 * width, WIDE), bf16),
            shape((turns, 1, WIDE), i32),
            shape((2 * span + 8, LANES), i32),
            shape((LANES, ex), f32),
            shape((8, ex), f32),
        ),
        in_specs=[ANY] * 5,
        out_specs=(VM, VM, VM, SM, VM, VM),
        scratch_shapes=[
            pltpu.VMEM((rows, width), f32),
            pltpu.VMEM((rows, width), bf16),
            pltpu.VMEM((slots, ex), i32),
            pltpu.VMEM((1, ex), i32),
            pltpu.VMEM((1, ex), i32),
            pltpu.VMEM((ex * grains, GRAIN, width), bf16),
            pltpu.VMEM((ex * grains + 8, LANES), i32),
            pltpu.VMEM((2 * span + 8, LANES), i32),
            pltpu.SMEM((2 * span + 8, LANES), i32),
            dma((deep - 1,)), dma((deep - 1,)), dma((deep,)), dma((deep,)), dma((7,)),
        ],
        compiler_params=pltpu.CompilerParams(collective_id=0, has_side_effects=True, vmem_limit_bytes=GRANT),
        cost_estimate=COST,
    )(*[
        pltpu.with_memory_space_constraint(a, pltpu.HBM)
        for a in (weights, tile_blocks.T, tile_counts.reshape(1, ex), owner_rank.reshape(1, ex), vals)
    ])

    partial = pl.pallas_call(
        margin_kernel,
        out_shape=shape((8, ex), f32),
        in_specs=[SM, VM, VM, VM],
        out_specs=VM,
        scratch_shapes=[pltpu.VMEM((ex * grains + 8, LANES), f32)],
        compiler_params=pltpu.CompilerParams(vmem_limit_bytes=GRANT),
        cost_estimate=COST,
    )(lists, table, x2, high)

    margin, resid, loss_part = pl.pallas_call(
        functools.partial(residual_kernel, nf),
        out_shape=(shape((8, ex), f32), shape((1, ex), f32), shape((8, LANES), f32)),
        in_specs=[VM, VM],
        out_specs=(VM, VM, VM),
        scratch_shapes=[pltpu.VMEM((nf, 8, ex), f32), dma((nf - 1,)), dma((nf - 1,))],
        compiler_params=pltpu.CompilerParams(collective_id=1, has_side_effects=True, vmem_limit_bytes=GRANT),
        cost_estimate=COST,
    )(partial, labels.reshape(1, ex))

    grad_part = pl.pallas_call(
        functools.partial(gradient_kernel, grains),
        out_shape=shape((n, rows, width), bf16),
        in_specs=[SM, SM, VM, VM],
        out_specs=VM,
        scratch_shapes=[pltpu.VMEM((deep * rows, 2 * width), f32)],
        compiler_params=pltpu.CompilerParams(vmem_limit_bytes=GRANT),
        cost_estimate=COST,
    )(lists, resid, x2, high)

    total, notes = pl.pallas_call(
        functools.partial(scatter_kernel, n),
        out_shape=(shape((rows, width), f32), shape((n, 8, LANES), f32)),
        in_specs=[VM] * 5,
        out_specs=(VM, VM),
        scratch_shapes=[
            pltpu.VMEM((n, 8, LANES), f32),
            pltpu.VMEM((deep, rows, width), bf16),
            pltpu.VMEM((deep - 1, rows, width), bf16),
            pltpu.VMEM((deep - 1, rows, width), bf16),
            dma((deep - 1,)),
            dma((deep - 1,)),
            dma((deep,)),
            dma((deep,)),
            dma((n - 1,)),
            dma((n - 1,)),
        ],
        compiler_params=pltpu.CompilerParams(collective_id=2, has_side_effects=True, vmem_limit_bytes=GRANT),
        cost_estimate=COST,
    )(grad_part, margin, owner, rank, loss_part)

    owned, gradient, loss = pl.pallas_call(
        finish_kernel,
        out_shape=(shape((1, ex), f32), shape((rows, width), f32), shape((1, 1), f32)),
        in_specs=[VM, VM],
        out_specs=(VM, VM, SM),
        compiler_params=pltpu.CompilerParams(vmem_limit_bytes=GRANT),
        cost_estimate=COST,
    )(total, notes)
    return owned.reshape(ex), gradient, loss.reshape(())


def solution(mesh):
    in_specs = (
        P("rows", "feat", None),
        P("rows", "feat"),
        P("rows", "feat"),
        P("rows"),
        P("rows"),
        P(("feat", "rows"), None),
    )
    out_specs = (P("rows"), P(("feat", "rows"), None), P())
    body = functools.partial(on_device, mesh.shape["rows"], mesh.shape["feat"])
    return jax.shard_map(body, mesh=mesh, in_specs=in_specs, out_specs=out_specs, check_vma=False)
```

```python
import functools

import jax
import jax.numpy as jnp
from jax import lax
from jax.experimental import pallas as pl
from jax.experimental.pallas import tpu as pltpu
from jax.sharding import PartitionSpec as P

MESH = pl.DeviceIdType.MESH
LANES = 128
GRAIN = 16
GROUP = 32
GRANT = 24 * 1024 * 1024
COST = pl.CostEstimate(flops=0, bytes_accessed=24 * 1024 * 1024, transcendentals=0)
NT = (((1,), (1,)), ((), ()))
NN = (((1,), (0,)), ((), ()))
VM = pl.BlockSpec(memory_space=pltpu.VMEM)
SM = pl.BlockSpec(memory_space=pltpu.SMEM)
ANY = pl.BlockSpec(memory_space=pltpu.HBM)
WIDE = GROUP * GRAIN
PER = LANES // GRAIN
CUT = 256


def seat(n):
    me = lax.axis_index("rows")
    side = lax.rem(me, 2)
    spot = me // 2
    partner = me + 1 - 2 * side
    deep = n // 2
    tables = [sorted((z for z in range(deep) if z != at), key=lambda z: -abs(z - at)) for at in range(deep)]
    far = []
    for j in range(deep - 1):
        pick = tables[0][j]
        for at in range(1, deep):
            pick = pick + (tables[at][j] - tables[at - 1][j]) * ((spot + deep - at) // deep)
        far.append(pick)
    return me, side, spot, partner, far


def call_out(axis, peers):
    barrier = pltpu.get_barrier_semaphore()
    for peer in peers:
        pl.semaphore_signal(barrier, inc=1, device_id={axis: peer}, device_id_type=MESH)
    return lambda: pl.semaphore_wait(barrier, len(peers))


def copy_to(axis, peer, source, target, send, recv):
    return pltpu.make_async_remote_copy(
        src_ref=source,
        dst_ref=target,
        send_sem=send,
        recv_sem=recv,
        device_id={axis: peer},
        device_id_type=MESH,
    )


def send_to(*args):
    copy = copy_to(*args)
    copy.start()
    return copy


def lane_group():
    return lax.broadcasted_iota(jnp.int32, (1, LANES), 1) // GRAIN


def own_lanes():
    sub = lax.broadcasted_iota(jnp.int32, (8, LANES), 0)
    return sub == lax.broadcasted_iota(jnp.int32, (8, LANES), 1) // GRAIN


def offsets(row):
    return jnp.broadcast_to(row, (8, WIDE)) - lax.broadcasted_iota(jnp.int32, (8, WIDE), 0)


def select_scores(pair, x2, offset, first, found):
    scores = lax.dot_general(pair, x2, NN, preferred_element_type=jnp.float32)
    for i in range(pair.shape[0] // 8):
        found = jnp.where(offset == first + i * 8, scores[i * 8 : i * 8 + 8, :], found)
    return found


def spread_sum(x2, offset, factor, first, rows):
    spread = jnp.concatenate(
        [jnp.where(offset == first + i * 8, factor, 0.0) for i in range(rows // 8)], axis=0
    ).astype(jnp.bfloat16)
    return lax.dot_general(spread, x2, NT, preferred_element_type=jnp.float32)


def gather_kernel(
    n, w_hbm, ids_hbm, used_hbm, owner_hbm, vals_hbm,
    table_ref, x2_ref, hi_ref, lists_ref, rank_ref, owner_ref, first_ref,
    w_buf, half, ids, used, own, vals, idt, lists, glist, found,
    send, recv, xsend, xrecv, here,
):
    local = [
        pltpu.make_async_copy(w_hbm, w_buf, here.at[0]),
        pltpu.make_async_copy(used_hbm, used, here.at[1]),
        pltpu.make_async_copy(ids_hbm, ids, here.at[2]),
        pltpu.make_async_copy(owner_hbm, own, here.at[3]),
        pltpu.make_async_copy(vals_hbm, vals, here.at[4]),
    ]
    for copy in local:
        copy.start()
    me, side, spot, partner, far = seat(n)
    deep = n // 2
    rows = w_buf.shape[0]
    slots, ex = ids.shape
    grains = slots // GRAIN
    joined = call_out("rows", [partner] + [2 * z + side for z in far])
    local[0].wait()
    half[...] = w_buf[...].astype(jnp.bfloat16)
    joined()
    across = [send_to("rows", partner, half, table_ref.at[me], xsend.at[spot], xrecv.at[spot])]
    along = [
        send_to("rows", 2 * z + side, half, table_ref.at[me], send.at[j], recv.at[spot])
        for j, z in enumerate(far)
    ]
    table_ref[me] = w_buf[...].astype(jnp.bfloat16)

    f32 = jnp.float32
    local[1].wait()
    count = (used[...] + (GRAIN - 1)) // GRAIN - 1
    sizes = jnp.broadcast_to(count, (LANES, ex)).T
    down = lax.broadcasted_iota(jnp.int32, (ex, LANES), 0)
    ends = sizes
    step = 1
    while step < ex:
        ends = ends + jnp.where(down >= step, pltpu.roll(ends, step, 0), 0)
        step *= 2
    lane = lax.broadcasted_iota(jnp.int32, (1, LANES), 1)
    span = ex * (grains - 1) // LANES
    hold = lists.shape[0] // 3
    for b in range(span):
        place = lane + b * LANES
        past = ends <= place
        which = jnp.sum(jnp.where(past, 1, 0), axis=0, keepdims=True)
        begin = jnp.sum(jnp.where(past, sizes, 0), axis=0, keepdims=True)
        live = which < ex
        q = place - begin + 1
        lists[b : b + 1, :] = jnp.clip(jnp.where(live, which * grains + q, 0), 0, grains * ex - 1)
        lists[hold + b : hold + b + 1, :] = jnp.clip(jnp.where(live, which + q * ex, grains * ex), 0, grains * ex)
    turns = (ends[ex - 8 : ex, :] + (GROUP - 1)) // GROUP
    lists[2 * hold :, :] = jnp.broadcast_to(turns[7:8, :], (hold, LANES))
    to_list = pltpu.make_async_copy(lists, glist, here.at[5])
    to_list.start()
    to_next = pltpu.make_async_copy(lists, lists_ref, here.at[6])
    to_next.start()

    local[2].wait()
    live = lax.broadcasted_iota(jnp.int32, (slots, ex), 0) < used[...]
    shifted = jnp.where(live, ids[...] + 1, 0)
    if slots < LANES:
        shifted = jnp.concatenate([shifted, jnp.zeros((LANES - slots, ex), jnp.int32)], axis=0)
    shifted = shifted.T
    grain_of = lax.broadcasted_iota(jnp.int32, (ex, LANES), 1) // GRAIN
    for q in range(grains):
        piece = jnp.where(grain_of == q, shifted, 0)
        step = GRAIN
        while step < LANES:
            piece = piece + pltpu.roll(piece, step, 1)
            step *= 2
        idt[q * ex : (q + 1) * ex, :] = piece - 1
    idt[grains * ex :, :] = jnp.full((8, LANES), -1, jnp.int32)

    tall = x2_ref.shape[1] // 2

    def put(t, values, id_row):
        chunk = id_row // rows
        odd = lax.rem(chunk, 2)
        high = jnp.where(id_row < 0, -1, (chunk // 2) * rows + lax.rem(id_row, rows))
        hi_ref[t] = high
        odd = jnp.broadcast_to(odd.astype(f32), (16, WIDE))
        odd_half = jnp.concatenate([odd.astype(jnp.bfloat16)] * (tall // 16), axis=0)
        even_half = jnp.concatenate([(1.0 - odd).astype(jnp.bfloat16)] * (tall // 16), axis=0)
        flipped = values.T
        x2_ref[t, 0:tall, :] = flipped * even_half
        x2_ref[t, tall:, :] = flipped * odd_half

    mine = own_lanes()
    group = lane_group()
    steady = ex // GROUP

    def prepare_first(t, carry):
        at = t * GROUP
        values = jnp.concatenate([vals[(at + i) * grains] for i in range(GROUP)], axis=0)
        parts = [
            jnp.sum(jnp.where(mine, idt[pl.ds(at + h * PER, PER), :], 0), axis=0, keepdims=True)
            for h in range(GROUP // PER)
        ]
        put(t, values, jnp.concatenate(parts, axis=1))
        found[t] = jnp.zeros((8, WIDE), f32)
        return carry

    def prepare_rest(t, carry):
        row = t * GROUP // LANES
        col = lax.rem(t * GROUP, LANES)
        values = jnp.concatenate([vals[glist[row, col + i]] for i in range(GROUP)], axis=0)
        parts = []
        for h in range(GROUP // PER):
            line = idt[pl.ds(glist[hold + row, col + h * PER], 1), :]
            for i in range(1, PER):
                line = jnp.where(group == i, idt[pl.ds(glist[hold + row, col + h * PER + i], 1), :], line)
            parts.append(line)
        put(steady + t, values, jnp.concatenate(parts, axis=1))
        return carry

    def score(z):
        pair = jnp.concatenate([table_ref[2 * z], table_ref[2 * z + 1]], axis=1)

        def turn(t, carry):
            found[t] = select_scores(pair, x2_ref[t], offsets(hi_ref[t]), z * rows, found[t])
            return carry

        lax.fori_loop(0, steady, turn, jnp.int32(0), unroll=2)

    local[4].wait()
    lax.fori_loop(0, steady, prepare_first, jnp.int32(0), unroll=2)
    to_list.wait()
    to_next.wait()

    def arrival(z):
        return copy_to("rows", partner, half, table_ref.at[2 * z + side], send.at[0], recv.at[z])

    def crossing(z):
        return copy_to("rows", partner, half, table_ref.at[2 * z + 1 - side], send.at[0], xrecv.at[z])

    near = far[::-1]
    total = x2_ref.shape[0] - steady
    cuts = [total * j // (deep - 1) for j in range(deep)]
    cuts = [c // 2 * 2 for c in cuts[:-1]] + [total]
    for j, z in enumerate(near):
        arrival(z).wait_recv()
        block = table_ref.at[2 * z + side]
        across.append(send_to("rows", partner, block, block, xsend.at[z], xrecv.at[z]))
        lax.fori_loop(cuts[j], cuts[j + 1], prepare_rest, jnp.int32(0), unroll=2 if deep == 4 else 1)
        done = spot if j == 0 else near[j - 1]
        crossing(done).wait_recv()
        score(done)

    local[3].wait()
    owner = own[...].astype(f32)
    square = jnp.broadcast_to(owner, (ex, ex))
    earlier = lax.broadcasted_iota(jnp.int32, (ex, ex), 0) < lax.broadcasted_iota(jnp.int32, (ex, ex), 1)
    same = jnp.where(jnp.logical_and(square.T == square, earlier), 1.0, 0.0)
    shift = lax.rem(me * (ex // n), LANES).astype(f32)
    rank = jnp.sum(same, axis=0, keepdims=True) + shift
    places = lax.broadcasted_iota(jnp.int32, (LANES, ex), 0).astype(f32)
    rank_ref[...] = jnp.where(places == rank, 1.0, 0.0)
    owner_ref[...] = jnp.broadcast_to(owner, owner_ref.shape)

    crossing(near[-1]).wait_recv()
    score(near[-1])
    for t in range(steady):
        term = jnp.sum(found[t], axis=0, keepdims=True)
        for h in range(GROUP // PER):
            at = t * GROUP + h * PER
            first_ref[at : at + PER, :] = jnp.where(mine, term[:, h * LANES : (h + 1) * LANES], 0.0)
    for copy in along:
        copy.wait_send()
    for copy in across:
        copy.wait_send()


def margin_kernel(lists, table_ref, x2_ref, hi_ref, first_ref, partial_ref, terms):
    n, rows, _ = table_ref.shape
    ex = partial_ref.shape[1]
    grains = terms.shape[0] // ex
    hold = lists.shape[0] // 3
    steady = ex // GROUP
    terms[ex:, :] = jnp.zeros((terms.shape[0] - ex, LANES), jnp.float32)
    group = lane_group()

    def one(t):
        x2 = x2_ref[steady + t]
        offset = offsets(hi_ref[steady + t])
        found = jnp.zeros((8, WIDE), jnp.float32)
        for k in range(n // 2):
            pair = jnp.concatenate([table_ref[2 * k], table_ref[2 * k + 1]], axis=1)
            found = select_scores(pair, x2, offset, k * rows, found)
        return jnp.sum(found, axis=0, keepdims=True)

    def keep(t, term):
        row = t * GROUP // LANES
        col = lax.rem(t * GROUP, LANES)
        for i in range(GROUP):
            h = i // PER
            mine = jnp.where(group == i % PER, term[:, h * LANES : (h + 1) * LANES], 0.0)
            terms[pl.ds(lists[hold + row, col + i], 1), :] = mine

    def turn(t, carry):
        a = one(2 * t)
        b = one(2 * t + 1)
        keep(2 * t, a)
        keep(2 * t + 1, b)
        return carry

    lax.fori_loop(0, (lists[2 * hold, 0] + 1) // 2, turn, jnp.int32(0))
    spread = first_ref[...]
    for q in range(1, grains):
        spread = spread + terms[q * ex : (q + 1) * ex, :]
    partial_ref[...] = jnp.broadcast_to(jnp.sum(spread.T, axis=0, keepdims=True), partial_ref.shape)


def residual_kernel(n, partial_ref, labels_ref, margin_ref, resid_ref, loss_ref, held, send, recv):
    me = lax.axis_index("feat")
    peers = [lax.rem(me + k, n) for k in range(1, n)]
    call_out("feat", peers)()
    copies = [
        send_to("feat", peer, partial_ref, held.at[me], send.at[k], recv.at[k])
        for k, peer in enumerate(peers)
    ]
    held[me] = partial_ref[...]
    for copy in copies:
        copy.wait()
    margin = held[0]
    for k in range(1, n):
        margin = margin + held[k]
    label = labels_ref[...].astype(jnp.float32)
    residual = 1.0 / (1.0 + jnp.exp(-margin)) - label
    margin_ref[...] = margin
    resid_ref[...] = residual.astype(jnp.bfloat16).astype(jnp.float32)[0:1, :]
    term = jnp.maximum(margin, 0.0) + jnp.log1p(jnp.exp(-jnp.abs(margin))) - label * margin
    total = term[:, 0:LANES]
    for h in range(1, term.shape[1] // LANES):
        total = total + term[:, h * LANES : (h + 1) * LANES]
    loss_ref[...] = total


def rest_kernel(grains, lists, resid, x2_ref, hi_ref, total):
    total[...] = jnp.zeros_like(total)
    hold = lists.shape[0] // 3
    rows = CUT
    steady = resid.shape[1] // GROUP
    group = lane_group()

    def turn(t, carry):
        x2 = x2_ref[steady + t]
        offset = offsets(hi_ref[steady + t])
        row_at = t * GROUP // LANES
        col = lax.rem(t * GROUP, LANES)
        parts = []
        for h in range(GROUP // PER):
            row = jnp.zeros((1, LANES), jnp.float32)
            for i in range(PER):
                row = jnp.where(group == i, resid[0, lists[row_at, col + h * PER + i] // grains], row)
            parts.append(row)
        factor = jnp.broadcast_to(jnp.concatenate(parts, axis=1), (8, WIDE))
        for k in range(total.shape[0] // rows):
            total[k * rows : (k + 1) * rows, :] += spread_sum(x2, offset, factor, k * rows, rows)
        return carry

    lax.fori_loop(0, lists[2 * hold, 0], turn, jnp.int32(0))


def scatter_kernel(
    n, rest_ref, resid_ref, x2_ref, hi_ref, margin_ref, owner_ref, rank_ref, loss_ref,
    sum_ref, notes_ref,
    notes, factors, acc, part, crossed, paired, held, send, recv, xsend, xrecv, nsend, nrecv,
):
    ex = margin_ref.shape[1]
    me, side, spot, partner, far = seat(n)
    deep = n // 2
    rows, width = sum_ref.shape
    others = [lax.rem(me + k, n) for k in range(1, n)]
    joined = call_out("rows", others)
    mine = own_lanes()
    steady = ex // GROUP
    tall = jnp.broadcast_to(resid_ref[...], (LANES, ex)).T
    for t in range(steady):
        parts = [
            jnp.sum(
                jnp.where(mine, tall[t * GROUP + h * PER : t * GROUP + (h + 1) * PER, :], 0.0), axis=0, keepdims=True
            )
            for h in range(GROUP // PER)
        ]
        factors[t] = jnp.concatenate(parts, axis=1)

    def gather_pair(j, z):
        acc[...] = rest_ref[pl.ds(pl.multiple_of(z * rows, rows), rows), :]

        def turn(t, carry):
            factor = jnp.broadcast_to(factors[t], (8, WIDE))
            acc[...] += spread_sum(x2_ref[t], offsets(hi_ref[t]), factor, z * rows, rows)
            return carry

        lax.fori_loop(0, steady, turn, jnp.int32(0), unroll=2)
        part[j, 0] = acc[:, 0:width].astype(jnp.bfloat16)
        part[j, 1] = acc[:, width:].astype(jnp.bfloat16)

    def cross(j):
        return send_to("rows", partner, part.at[j, 1 - side], crossed.at[j], xsend.at[j], xrecv.at[j])

    across = []
    along = []

    def pass_on(j):
        across[j].wait_recv()
        pair = part[j, side].astype(jnp.float32) + crossed[j].astype(jnp.float32)
        paired[j] = pair.astype(jnp.bfloat16)
        along.append(
            send_to("rows", 2 * far[j] + side, paired.at[j], held.at[spot], send.at[j], recv.at[spot])
        )

    last = deep - 1
    lead = deep - 2
    gather_pair(0, far[0])
    joined()
    across.append(cross(0))
    for j in range(1, deep):
        gather_pair(j, far[j] if j < last else spot)
        across.append(cross(j))
        if j >= lead:
            pass_on(j - lead)

    which = lax.broadcasted_iota(jnp.int32, (n, ex), 0).astype(jnp.float32)
    by_owner = jnp.where(which == owner_ref[0:1, :], margin_ref[0:1, :], 0.0)
    ordered = lax.dot_general(
        by_owner, rank_ref[...], NT, precision=lax.Precision.HIGHEST, preferred_element_type=jnp.float32
    )
    sub = lax.broadcasted_iota(jnp.int32, (8, LANES), 0)
    for d in range(n):
        notes[d] = jnp.where(sub == 0, ordered[d : d + 1, :], loss_ref[...])
    told = [
        send_to("rows", peer, notes.at[peer], notes_ref.at[me], nsend.at[k], nrecv.at[k])
        for k, peer in enumerate(others)
    ]
    notes_ref[me] = notes[me]
    for j in range(last - lead + 1, last):
        pass_on(j)
    across[last].wait_recv()
    total = part[last, side].astype(jnp.float32) + crossed[last].astype(jnp.float32)
    for z in far[::-1]:
        copy_to("rows", partner, paired.at[0], held.at[z], send.at[0], recv.at[z]).wait_recv()
        total = total + held[z].astype(jnp.float32)
    sum_ref[...] = total
    for copy in across:
        copy.wait_send()
    for copy in along:
        copy.wait_send()
    for copy in told:
        copy.wait()


def finish_kernel(sum_ref, notes_ref, owned_ref, grad_ref, loss_ref):
    n = notes_ref.shape[0]
    ex = owned_ref.shape[1]
    grad_ref[...] = sum_ref[...]
    for h in range(ex // LANES):
        row = jnp.zeros((1, LANES), jnp.float32)
        for d in range(n):
            if d * (ex // n) // LANES == h:
                row = row + notes_ref[d, 0:1, :]
        owned_ref[:, h * LANES : (h + 1) * LANES] = row
    loss = jnp.zeros((1, LANES), jnp.float32)
    for d in range(n):
        loss = loss + notes_ref[d, 1:2, :]
    loss_ref[0, 0] = jnp.sum(loss) * (1.0 / (ex * n))


def on_device(n, nf, tile_values, tile_blocks, tile_counts, labels, owner_rank, weights):
    ex, slots, width = tile_values.shape
    grains = slots // GRAIN
    rows = weights.shape[0]
    deep = n // 2
    turns = ex * grains // GROUP
    steady = ex // GROUP
    hold = -(-(ex * (grains - 1)) // (8 * LANES)) * 8
    f32, i32, bf16 = jnp.float32, jnp.int32, jnp.bfloat16
    shape = jax.ShapeDtypeStruct
    dma = pltpu.SemaphoreType.DMA
    vals = tile_values.reshape(ex * grains, GRAIN, width)

    table, x2, high, lists, rank, owner, first = pl.pallas_call(
        functools.partial(gather_kernel, n),
        out_shape=(
            shape((n, rows, width), bf16),
            shape((turns, 2 * width, WIDE), bf16),
            shape((turns, 1, WIDE), i32),
            shape((3 * hold, LANES), i32),
            shape((LANES, ex), f32),
            shape((8, ex), f32),
            shape((ex, LANES), f32),
        ),
        in_specs=[ANY] * 5,
        out_specs=(VM, VM, VM, SM, VM, VM, VM),
        scratch_shapes=[
            pltpu.VMEM((rows, width), f32),
            pltpu.VMEM((rows, width), bf16),
            pltpu.VMEM((slots, ex), i32),
            pltpu.VMEM((1, ex), i32),
            pltpu.VMEM((1, ex), i32),
            pltpu.VMEM((ex * grains, GRAIN, width), bf16),
            pltpu.VMEM((ex * grains + 8, LANES), i32),
            pltpu.VMEM((3 * hold, LANES), i32),
            pltpu.SMEM((3 * hold, LANES), i32),
            pltpu.VMEM((steady, 8, WIDE), f32),
            dma((deep - 1,)), dma((deep,)), dma((deep,)), dma((deep,)), dma((7,)),
        ],
        compiler_params=pltpu.CompilerParams(collective_id=0, has_side_effects=True, vmem_limit_bytes=GRANT),
        cost_estimate=COST,
    )(*[
        pltpu.with_memory_space_constraint(a, pltpu.HBM)
        for a in (weights, tile_blocks.T, tile_counts.reshape(1, ex), owner_rank.reshape(1, ex), vals)
    ])

    partial = pl.pallas_call(
        margin_kernel,
        out_shape=shape((8, ex), f32),
        in_specs=[SM, VM, VM, VM, VM],
        out_specs=VM,
        scratch_shapes=[pltpu.VMEM((ex * grains + 8, LANES), f32)],
        compiler_params=pltpu.CompilerParams(vmem_limit_bytes=GRANT),
        cost_estimate=COST,
    )(lists, table, x2, high, first)

    margin, resid, loss_part = pl.pallas_call(
        functools.partial(residual_kernel, nf),
        out_shape=(shape((8, ex), f32), shape((1, ex), f32), shape((8, LANES), f32)),
        in_specs=[VM, VM],
        out_specs=(VM, VM, VM),
        scratch_shapes=[pltpu.VMEM((nf, 8, ex), f32), dma((nf - 1,)), dma((nf - 1,))],
        compiler_params=pltpu.CompilerParams(collective_id=1, has_side_effects=True, vmem_limit_bytes=GRANT),
        cost_estimate=COST,
    )(partial, labels.reshape(1, ex))

    rest = pl.pallas_call(
        functools.partial(rest_kernel, grains),
        out_shape=shape((deep * rows, 2 * width), f32),
        in_specs=[SM, SM, VM, VM],
        out_specs=VM,
        compiler_params=pltpu.CompilerParams(vmem_limit_bytes=GRANT),
        cost_estimate=COST,
    )(lists, resid, x2, high)

    total, notes = pl.pallas_call(
        functools.partial(scatter_kernel, n),
        out_shape=(shape((rows, width), f32), shape((n, 8, LANES), f32)),
        in_specs=[VM] * 8,
        out_specs=(VM, VM),
        scratch_shapes=[
            pltpu.VMEM((n, 8, LANES), f32),
            pltpu.VMEM((steady, 1, WIDE), f32),
            pltpu.VMEM((rows, 2 * width), f32),
            pltpu.VMEM((deep, 2, rows, width), bf16),
            pltpu.VMEM((deep, rows, width), bf16),
            pltpu.VMEM((deep - 1, rows, width), bf16),
            pltpu.VMEM((deep, rows, width), bf16),
            dma((deep - 1,)),
            dma((deep,)),
            dma((deep,)),
            dma((deep,)),
            dma((n - 1,)),
            dma((n - 1,)),
        ],
        compiler_params=pltpu.CompilerParams(collective_id=2, has_side_effects=True, vmem_limit_bytes=GRANT),
        cost_estimate=COST,
    )(rest, resid, x2, high, margin, owner, rank, loss_part)

    owned, gradient, loss = pl.pallas_call(
        finish_kernel,
        out_shape=(shape((1, ex), f32), shape((rows, width), f32), shape((1, 1), f32)),
        in_specs=[VM, VM],
        out_specs=(VM, VM, SM),
        compiler_params=pltpu.CompilerParams(vmem_limit_bytes=GRANT),
        cost_estimate=COST,
    )(total, notes)
    return owned.reshape(ex), gradient, loss.reshape(())


def solution(mesh):
    in_specs = (
        P("rows", "feat", None),
        P("rows", "feat"),
        P("rows", "feat"),
        P("rows"),
        P("rows"),
        P(("feat", "rows"), None),
    )
    out_specs = (P("rows"), P(("feat", "rows"), None), P())
    body = functools.partial(on_device, mesh.shape["rows"], mesh.shape["feat"])
    return jax.shard_map(body, mesh=mesh, in_specs=in_specs, out_specs=out_specs, check_vma=False)
```

```python
import functools

import jax
import jax.numpy as jnp
from jax import lax
from jax.experimental import pallas as pl
from jax.experimental.pallas import tpu as pltpu
from jax.sharding import PartitionSpec as P

MESH = pl.DeviceIdType.MESH
LANES = 128
GRAIN = 16
GROUP = 32
GRANT = 24 * 1024 * 1024
COST = pl.CostEstimate(flops=0, bytes_accessed=24 * 1024 * 1024, transcendentals=0)
NT = (((1,), (1,)), ((), ()))
NN = (((1,), (0,)), ((), ()))
VM = pl.BlockSpec(memory_space=pltpu.VMEM)
SM = pl.BlockSpec(memory_space=pltpu.SMEM)
ANY = pl.BlockSpec(memory_space=pltpu.HBM)
WIDE = GROUP * GRAIN
PER = LANES // GRAIN
CUT = 256
TOGETHER = 2


def seat(n):
    me = lax.axis_index("rows")
    side = lax.rem(me, 2)
    spot = me // 2
    partner = me + 1 - 2 * side
    deep = n // 2

    def listed(key):
        tables = [sorted((z for z in range(deep) if z != at), key=functools.partial(key, at)) for at in range(deep)]
        out = []
        for j in range(deep - 1):
            pick = tables[0][j]
            for at in range(1, deep):
                pick = pick + (tables[at][j] - tables[at - 1][j]) * ((spot + deep - at) // deep)
            out.append(pick)
        return out

    far = listed(lambda at, z: -abs(z - at))
    first = listed(lambda at, z: (abs(z - at)!=1, -abs(z - at)))
    return me, side, spot, partner, far, first


def call_out(axis, peers):
    barrier = pltpu.get_barrier_semaphore()
    for peer in peers:
        pl.semaphore_signal(barrier, inc=1, device_id={axis: peer}, device_id_type=MESH)
    return lambda: pl.semaphore_wait(barrier, len(peers))


def copy_to(axis, peer, source, target, send, recv):
    return pltpu.make_async_remote_copy(
        src_ref=source,
        dst_ref=target,
        send_sem=send,
        recv_sem=recv,
        device_id={axis: peer},
        device_id_type=MESH,
    )


def send_to(*args):
    copy = copy_to(*args)
    copy.start()
    return copy


def lane_group():
    return lax.broadcasted_iota(jnp.int32, (1, LANES), 1) // GRAIN


def own_lanes():
    sub = lax.broadcasted_iota(jnp.int32, (8, LANES), 0)
    return sub == lax.broadcasted_iota(jnp.int32, (8, LANES), 1) // GRAIN


def offsets(row):
    return jnp.broadcast_to(row, (8, WIDE)) - lax.broadcasted_iota(jnp.int32, (8, WIDE), 0)


def select_scores(pair, x2, offset, first, found):
    scores = lax.dot_general(pair, x2, NN, preferred_element_type=jnp.float32)
    for i in range(pair.shape[0] // 8):
        found = jnp.where(offset == first + i * 8, scores[i * 8 : i * 8 + 8, :], found)
    return found


def spread_sum(x2, offset, factor, firsts, rows):
    spread = jnp.concatenate(
        [jnp.where(offset == first + i * 8, factor, 0.0) for first in firsts for i in range(rows // 8)], axis=0
    ).astype(jnp.bfloat16)
    return lax.dot_general(spread, x2, NT, preferred_element_type=jnp.float32)


def put(x2_ref, hi_ref, t, values, id_row, rows):
    tall = x2_ref.shape[1] // 2
    chunk = id_row // rows
    odd = lax.rem(chunk, 2)
    hi_ref[t] = jnp.where(id_row < 0, -1, (chunk // 2) * rows + lax.rem(id_row, rows))
    odd = jnp.broadcast_to(odd.astype(jnp.float32), (16, WIDE))
    odd_half = jnp.concatenate([odd.astype(jnp.bfloat16)] * (tall // 16), axis=0)
    even_half = jnp.concatenate([(1.0 - odd).astype(jnp.bfloat16)] * (tall // 16), axis=0)
    flipped = values.T
    x2_ref[t, 0:tall, :] = flipped * even_half
    x2_ref[t, tall:, :] = flipped * odd_half


def listed_tiles(vals, idt, lists, t):
    hold = lists.shape[0] // 3
    row = t * GROUP // LANES
    col = lax.rem(t * GROUP, LANES)
    group = lane_group()
    values = jnp.concatenate([vals[lists[row, col + i]] for i in range(GROUP)], axis=0)
    parts = []
    for h in range(GROUP // PER):
        line = idt[pl.ds(lists[hold + row, col + h * PER], 1), :]
        for i in range(1, PER):
            line = jnp.where(group == i, idt[pl.ds(lists[hold + row, col + h * PER + i], 1), :], line)
        parts.append(line)
    return values, jnp.concatenate(parts, axis=1)


def gather_kernel(
    n, w_hbm, ids_hbm, used_hbm, owner_hbm, vals_hbm,
    table_ref, x2_ref, hi_ref, lists_ref, rank_ref, owner_ref, first_ref, vals, idt,
    w_buf, half, ids, used, own, lists, glist, found,
    send, recv, xsend, xrecv, here,
):
    local = [
        pltpu.make_async_copy(w_hbm, w_buf, here.at[0]),
        pltpu.make_async_copy(used_hbm, used, here.at[1]),
        pltpu.make_async_copy(ids_hbm, ids, here.at[2]),
        pltpu.make_async_copy(owner_hbm, own, here.at[3]),
        pltpu.make_async_copy(vals_hbm, vals, here.at[4]),
    ]
    for copy in local:
        copy.start()
    me, side, spot, partner, far, first = seat(n)
    deep = n // 2
    rows = w_buf.shape[0]
    slots, ex = ids.shape
    grains = slots // GRAIN
    joined = call_out("rows", [partner] + [2 * z + side for z in far])
    local[0].wait()
    half[...] = w_buf[...].astype(jnp.bfloat16)
    joined()
    across = [send_to("rows", partner, half, table_ref.at[me], xsend.at[spot], xrecv.at[spot])]
    along = [
        send_to("rows", 2 * z + side, half, table_ref.at[me], send.at[j], recv.at[spot])
        for j, z in enumerate(first)
    ]
    table_ref[me] = w_buf[...].astype(jnp.bfloat16)

    f32 = jnp.float32
    local[1].wait()
    count = (used[...] + (GRAIN - 1)) // GRAIN - 1
    sizes = jnp.broadcast_to(count, (LANES, ex)).T
    down = lax.broadcasted_iota(jnp.int32, (ex, LANES), 0)
    ends = sizes
    step = 1
    while step < ex:
        ends = ends + jnp.where(down >= step, pltpu.roll(ends, step, 0), 0)
        step *= 2
    lane = lax.broadcasted_iota(jnp.int32, (1, LANES), 1)
    span = ex * (grains - 1) // LANES
    hold = lists.shape[0] // 3
    for b in range(span):
        place = lane + b * LANES
        past = ends <= place
        which = jnp.sum(jnp.where(past, 1, 0), axis=0, keepdims=True)
        begin = jnp.sum(jnp.where(past, sizes, 0), axis=0, keepdims=True)
        live = which < ex
        q = place - begin + 1
        lists[b : b + 1, :] = jnp.clip(jnp.where(live, which * grains + q, 0), 0, grains * ex - 1)
        lists[hold + b : hold + b + 1, :] = jnp.clip(jnp.where(live, which + q * ex, grains * ex), 0, grains * ex)
    turns = (ends[ex - 8 : ex, :] + (GROUP - 1)) // GROUP
    lists[2 * hold :, :] = jnp.broadcast_to(turns[7:8, :], (hold, LANES))
    to_list = pltpu.make_async_copy(lists, glist, here.at[5])
    to_list.start()
    to_next = pltpu.make_async_copy(lists, lists_ref, here.at[6])
    to_next.start()

    local[2].wait()
    live = lax.broadcasted_iota(jnp.int32, (slots, ex), 0) < used[...]
    shifted = jnp.where(live, ids[...] + 1, 0)
    if slots < LANES:
        shifted = jnp.concatenate([shifted, jnp.zeros((LANES - slots, ex), jnp.int32)], axis=0)
    shifted = shifted.T
    grain_of = lax.broadcasted_iota(jnp.int32, (ex, LANES), 1) // GRAIN
    for q in range(grains):
        piece = jnp.where(grain_of == q, shifted, 0)
        step = GRAIN
        while step < LANES:
            piece = piece + pltpu.roll(piece, step, 1)
            step *= 2
        idt[q * ex : (q + 1) * ex, :] = piece - 1
    idt[grains * ex :, :] = jnp.full((8, LANES), -1, jnp.int32)

    mine = own_lanes()
    steady = ex // GROUP

    def prepare_first(t, carry):
        at = t * GROUP
        values = jnp.concatenate([vals[(at + i) * grains] for i in range(GROUP)], axis=0)
        parts = [
            jnp.sum(jnp.where(mine, idt[pl.ds(at + h * PER, PER), :], 0), axis=0, keepdims=True)
            for h in range(GROUP // PER)
        ]
        put(x2_ref, hi_ref, t, values, jnp.concatenate(parts, axis=1), rows)
        found[t] = jnp.zeros((8, WIDE), f32)
        return carry

    def prepare_rest(t, carry):
        values, id_row = listed_tiles(vals, idt, glist, t)
        put(x2_ref, hi_ref, steady + t, values, id_row, rows)
        return carry

    def score(z):
        pair = jnp.concatenate([table_ref[2 * z], table_ref[2 * z + 1]], axis=1)

        def turn(t, carry):
            found[t] = select_scores(pair, x2_ref[t], offsets(hi_ref[t]), z * rows, found[t])
            return carry

        lax.fori_loop(0, steady, turn, jnp.int32(0), unroll=2)

    local[4].wait()
    lax.fori_loop(0, steady, prepare_first, jnp.int32(0), unroll=2)
    to_list.wait()
    to_next.wait()

    def arrival(z):
        return copy_to("rows", partner, half, table_ref.at[2 * z + side], send.at[0], recv.at[z])

    def crossing(z):
        return copy_to("rows", partner, half, table_ref.at[2 * z + 1 - side], send.at[0], xrecv.at[z])

    near = far[::-1]
    lax.fori_loop(0, x2_ref.shape[0] - steady, prepare_rest, jnp.int32(0), unroll=2)
    for j, z in enumerate(near):
        arrival(z).wait_recv()
        block = table_ref.at[2 * z + side]
        across.append(send_to("rows", partner, block, block, xsend.at[z], xrecv.at[z]))
        if j == 0:
            crossing(spot).wait_recv()
            score(spot)

    local[3].wait()
    owner = own[...].astype(f32)
    square = jnp.broadcast_to(owner, (ex, ex))
    earlier = lax.broadcasted_iota(jnp.int32, (ex, ex), 0) < lax.broadcasted_iota(jnp.int32, (ex, ex), 1)
    same = jnp.where(jnp.logical_and(square.T == square, earlier), 1.0, 0.0)
    shift = lax.rem(me * (ex // n), LANES).astype(f32)
    rank = jnp.sum(same, axis=0, keepdims=True) + shift
    places = lax.broadcasted_iota(jnp.int32, (LANES, ex), 0).astype(f32)
    rank_ref[...] = jnp.where(places == rank, 1.0, 0.0)
    owner_ref[...] = jnp.broadcast_to(owner, owner_ref.shape)

    for z in near:
        crossing(z).wait_recv()
        score(z)
    for t in range(steady):
        term = jnp.sum(found[t], axis=0, keepdims=True)
        for h in range(GROUP // PER):
            at = t * GROUP + h * PER
            first_ref[at : at + PER, :] = jnp.where(mine, term[:, h * LANES : (h + 1) * LANES], 0.0)
    for copy in along:
        copy.wait_send()
    for copy in across:
        copy.wait_send()


def margin_kernel(
    lists, table_ref, x2_ref, hi_ref, first_ref, vals, idt, partial_ref, more_x2, more_hi, terms
):
    n, rows, _ = table_ref.shape
    ex = partial_ref.shape[1]
    grains = terms.shape[0] // ex
    hold = lists.shape[0] // 3
    steady = ex // GROUP
    ready = x2_ref.shape[0] - steady
    terms[ex:, :] = jnp.zeros((terms.shape[0] - ex, LANES), jnp.float32)
    group = lane_group()

    def one(x2, row):
        offset = offsets(row)
        found = jnp.zeros((8, WIDE), jnp.float32)
        for k in range(n // 2):
            pair = jnp.concatenate([table_ref[2 * k], table_ref[2 * k + 1]], axis=1)
            found = select_scores(pair, x2, offset, k * rows, found)
        return jnp.sum(found, axis=0, keepdims=True)

    def keep(t, term):
        row = t * GROUP // LANES
        col = lax.rem(t * GROUP, LANES)
        for i in range(GROUP):
            h = i // PER
            mine = jnp.where(group == i % PER, term[:, h * LANES : (h + 1) * LANES], 0.0)
            terms[pl.ds(lists[hold + row, col + i], 1), :] = mine

    def turn(t, carry):
        a = one(x2_ref[steady + 2 * t], hi_ref[steady + 2 * t])
        b = one(x2_ref[steady + 2 * t + 1], hi_ref[steady + 2 * t + 1])
        keep(2 * t, a)
        keep(2 * t + 1, b)
        return carry

    def late_turn(t, carry):
        values, id_row = listed_tiles(vals, idt, lists, t)
        put(more_x2, more_hi, t - ready, values, id_row, rows)
        keep(t, one(more_x2[t - ready], more_hi[t - ready]))
        return carry

    turns = lists[2 * hold, 0]
    lax.fori_loop(0, (jnp.minimum(turns, ready) + 1) // 2, turn, jnp.int32(0))
    lax.fori_loop(ready, turns, late_turn, jnp.int32(0))
    spread = first_ref[...]
    for q in range(1, grains):
        spread = spread + terms[q * ex : (q + 1) * ex, :]
    partial_ref[...] = jnp.broadcast_to(jnp.sum(spread.T, axis=0, keepdims=True), partial_ref.shape)


def residual_kernel(n, partial_ref, labels_ref, margin_ref, resid_ref, loss_ref, held, send, recv):
    me = lax.axis_index("feat")
    peers = [lax.rem(me + k, n) for k in range(1, n)]
    call_out("feat", peers)()
    copies = [
        send_to("feat", peer, partial_ref, held.at[me], send.at[k], recv.at[k])
        for k, peer in enumerate(peers)
    ]
    held[me] = partial_ref[...]
    for copy in copies:
        copy.wait()
    margin = held[0]
    for k in range(1, n):
        margin = margin + held[k]
    label = labels_ref[...].astype(jnp.float32)
    residual = 1.0 / (1.0 + jnp.exp(-margin)) - label
    margin_ref[...] = margin
    resid_ref[...] = residual.astype(jnp.bfloat16).astype(jnp.float32)[0:1, :]
    term = jnp.maximum(margin, 0.0) + jnp.log1p(jnp.exp(-jnp.abs(margin))) - label * margin
    total = term[:, 0:LANES]
    for h in range(1, term.shape[1] // LANES):
        total = total + term[:, h * LANES : (h + 1) * LANES]
    loss_ref[...] = total


def rest_kernel(grains, lists, resid, x2_ref, hi_ref, more_x2, more_hi, total):
    total[...] = jnp.zeros_like(total)
    hold = lists.shape[0] // 3
    rows = CUT
    steady = resid.shape[1] // GROUP
    ready = x2_ref.shape[0] - steady
    group = lane_group()

    def factor_of(t):
        row_at = t * GROUP // LANES
        col = lax.rem(t * GROUP, LANES)
        parts = []
        for h in range(GROUP // PER):
            row = jnp.zeros((1, LANES), jnp.float32)
            for i in range(PER):
                row = jnp.where(group == i, resid[0, lists[row_at, col + h * PER + i] // grains], row)
            parts.append(row)
        return jnp.broadcast_to(jnp.concatenate(parts, axis=1), (8, WIDE))

    def turn(t, carry):
        at = steady + 2 * t
        x2a, x2b = x2_ref[at], x2_ref[at + 1]
        offset_a, offset_b = offsets(hi_ref[at]), offsets(hi_ref[at + 1])
        factor_a, factor_b = factor_of(2 * t), factor_of(2 * t + 1)
        for k in range(total.shape[0] // rows):
            total[k * rows : (k + 1) * rows, :] += spread_sum(
                x2a, offset_a, factor_a, [k * rows], rows
            ) + spread_sum(x2b, offset_b, factor_b, [k * rows], rows)
        return carry

    def late_turn(t, carry):
        x2, offset, factor = more_x2[t - ready], offsets(more_hi[t - ready]), factor_of(t)
        for k in range(total.shape[0] // rows):
            total[k * rows : (k + 1) * rows, :] += spread_sum(x2, offset, factor, [k * rows], rows)
        return carry

    turns = lists[2 * hold, 0]
    lax.fori_loop(0, (jnp.minimum(turns, ready) + 1) // 2, turn, jnp.int32(0))
    lax.fori_loop(ready, turns, late_turn, jnp.int32(0))


def scatter_kernel(
    n, rest_ref, resid_ref, x2_ref, hi_ref, margin_ref, owner_ref, rank_ref, loss_ref,
    sum_ref, notes_ref,
    notes, factors, acc, part, crossed, paired, held, send, recv, xsend, xrecv, nsend, nrecv,
):
    ex = margin_ref.shape[1]
    me, side, spot, partner, far, first = seat(n)
    deep = n // 2
    rows, width = sum_ref.shape
    others = [lax.rem(me + k, n) for k in range(1, n)]
    joined = call_out("rows", others)
    mine = own_lanes()
    steady = ex // GROUP
    tall = jnp.broadcast_to(resid_ref[...], (LANES, ex)).T
    for t in range(steady):
        parts = [
            jnp.sum(
                jnp.where(mine, tall[t * GROUP + h * PER : t * GROUP + (h + 1) * PER, :], 0.0), axis=0, keepdims=True
            )
            for h in range(GROUP // PER)
        ]
        factors[t] = jnp.concatenate(parts, axis=1)

    def gather_pairs(js, zs):
        for i, z in enumerate(zs):
            acc[i * rows : (i + 1) * rows, :] = rest_ref[pl.ds(pl.multiple_of(z * rows, rows), rows), :]
        high = len(js) * rows

        def turn(t, carry):
            factor = jnp.broadcast_to(factors[t], (8, WIDE))
            acc[0:high, :] += spread_sum(x2_ref[t], offsets(hi_ref[t]), factor, [z * rows for z in zs], rows)
            return carry

        lax.fori_loop(0, steady, turn, jnp.int32(0), unroll=2)
        for i, j in enumerate(js):
            part[j, 0] = acc[i * rows : (i + 1) * rows, 0:width].astype(jnp.bfloat16)
            part[j, 1] = acc[i * rows : (i + 1) * rows, width:].astype(jnp.bfloat16)

    def cross(j):
        return send_to("rows", partner, part.at[j, 1 - side], crossed.at[j], xsend.at[j], xrecv.at[j])

    across = []
    along = []

    def pass_on(j):
        across[j].wait_recv()
        pair = part[j, side].astype(jnp.float32) + crossed[j].astype(jnp.float32)
        paired[j] = pair.astype(jnp.bfloat16)
        along.append(
            send_to("rows", 2 * far[j] + side, paired.at[j], held.at[spot], send.at[j], recv.at[spot])
        )

    last = deep - 1
    planes = far + [spot]
    for j in range(0, deep, TOGETHER):
        js = list(range(j, min(j + TOGETHER, deep)))
        gather_pairs(js, [planes[i] for i in js])
        if j == 0:
            joined()
        across += [cross(i) for i in js]

    which = lax.broadcasted_iota(jnp.int32, (n, ex), 0).astype(jnp.float32)
    by_owner = jnp.where(which == owner_ref[0:1, :], margin_ref[0:1, :], 0.0)
    ordered = lax.dot_general(
        by_owner, rank_ref[...], NT, precision=lax.Precision.HIGHEST, preferred_element_type=jnp.float32
    )
    sub = lax.broadcasted_iota(jnp.int32, (8, LANES), 0)
    for d in range(n):
        notes[d] = jnp.where(sub == 0, ordered[d : d + 1, :], loss_ref[...])
    told = [
        send_to("rows", peer, notes.at[peer], notes_ref.at[me], nsend.at[k], nrecv.at[k])
        for k, peer in enumerate(others)
    ]
    notes_ref[me] = notes[me]
    for j in range(last):
        pass_on(j)
    across[last].wait_recv()
    total = part[last, side].astype(jnp.float32) + crossed[last].astype(jnp.float32)
    for z in far[::-1]:
        copy_to("rows", partner, paired.at[0], held.at[z], send.at[0], recv.at[z]).wait_recv()
        total = total + held[z].astype(jnp.float32)
    sum_ref[...] = total
    for copy in across:
        copy.wait_send()
    for copy in along:
        copy.wait_send()
    for copy in told:
        copy.wait()


def finish_kernel(sum_ref, notes_ref, owned_ref, grad_ref, loss_ref):
    n = notes_ref.shape[0]
    ex = owned_ref.shape[1]
    grad_ref[...] = sum_ref[...]
    for h in range(ex // LANES):
        row = jnp.zeros((1, LANES), jnp.float32)
        for d in range(n):
            if d * (ex // n) // LANES == h:
                row = row + notes_ref[d, 0:1, :]
        owned_ref[:, h * LANES : (h + 1) * LANES] = row
    loss = jnp.zeros((1, LANES), jnp.float32)
    for d in range(n):
        loss = loss + notes_ref[d, 1:2, :]
    loss_ref[0, 0] = jnp.sum(loss) * (1.0 / (ex * n))


def on_device(n, nf, tile_values, tile_blocks, tile_counts, labels, owner_rank, weights):
    ex, slots, width = tile_values.shape
    grains = slots // GRAIN
    rows = weights.shape[0]
    deep = n // 2
    steady = ex // GROUP
    late = max((grains - 2) * steady, 1)
    hold = -(-(ex * (grains - 1)) // (8 * LANES)) * 8
    f32, i32, bf16 = jnp.float32, jnp.int32, jnp.bfloat16
    shape = jax.ShapeDtypeStruct
    dma = pltpu.SemaphoreType.DMA
    vals = tile_values.reshape(ex * grains, GRAIN, width)

    table, x2, high, lists, rank, owner, first, packed, named = pl.pallas_call(
        functools.partial(gather_kernel, n),
        out_shape=(
            shape((n, rows, width), bf16),
            shape((2 * steady, 2 * width, WIDE), bf16),
            shape((2 * steady, 1, WIDE), i32),
            shape((3 * hold, LANES), i32),
            shape((LANES, ex), f32),
            shape((8, ex), f32),
            shape((ex, LANES), f32),
            shape((ex * grains, GRAIN, width), bf16),
            shape((ex * grains + 8, LANES), i32),
        ),
        in_specs=[ANY] * 5,
        out_specs=(VM, VM, VM, SM, VM, VM, VM, VM, VM),
        scratch_shapes=[
            pltpu.VMEM((rows, width), f32),
            pltpu.VMEM((rows, width), bf16),
            pltpu.VMEM((slots, ex), i32),
            pltpu.VMEM((1, ex), i32),
            pltpu.VMEM((1, ex), i32),
            pltpu.VMEM((3 * hold, LANES), i32),
            pltpu.SMEM((3 * hold, LANES), i32),
            pltpu.VMEM((steady, 8, WIDE), f32),
            dma((deep - 1,)), dma((deep,)), dma((deep,)), dma((deep,)), dma((7,)),
        ],
        compiler_params=pltpu.CompilerParams(collective_id=0, has_side_effects=True, vmem_limit_bytes=GRANT),
        cost_estimate=COST,
    )(*[
        pltpu.with_memory_space_constraint(a, pltpu.HBM)
        for a in (weights, tile_blocks.T, tile_counts.reshape(1, ex), owner_rank.reshape(1, ex), vals)
    ])

    partial, more_x2, more_high = pl.pallas_call(
        margin_kernel,
        out_shape=(shape((8, ex), f32), shape((late, 2 * width, WIDE), bf16), shape((late, 1, WIDE), i32)),
        in_specs=[SM] + [VM] * 6,
        out_specs=(VM, VM, VM),
        scratch_shapes=[pltpu.VMEM((ex * grains + 8, LANES), f32)],
        compiler_params=pltpu.CompilerParams(vmem_limit_bytes=GRANT),
        cost_estimate=COST,
    )(lists, table, x2, high, first, packed, named)

    margin, resid, loss_part = pl.pallas_call(
        functools.partial(residual_kernel, nf),
        out_shape=(shape((8, ex), f32), shape((1, ex), f32), shape((8, LANES), f32)),
        in_specs=[VM, VM],
        out_specs=(VM, VM, VM),
        scratch_shapes=[pltpu.VMEM((nf, 8, ex), f32), dma((nf - 1,)), dma((nf - 1,))],
        compiler_params=pltpu.CompilerParams(collective_id=1, has_side_effects=True, vmem_limit_bytes=GRANT),
        cost_estimate=COST,
    )(partial, labels.reshape(1, ex))

    rest = pl.pallas_call(
        functools.partial(rest_kernel, grains),
        out_shape=shape((deep * rows, 2 * width), f32),
        in_specs=[SM, SM, VM, VM, VM, VM],
        out_specs=VM,
        compiler_params=pltpu.CompilerParams(vmem_limit_bytes=GRANT),
        cost_estimate=COST,
    )(lists, resid, x2, high, more_x2, more_high)

    total, notes = pl.pallas_call(
        functools.partial(scatter_kernel, n),
        out_shape=(shape((rows, width), f32), shape((n, 8, LANES), f32)),
        in_specs=[VM] * 8,
        out_specs=(VM, VM),
        scratch_shapes=[
            pltpu.VMEM((n, 8, LANES), f32),
            pltpu.VMEM((steady, 1, WIDE), f32),
            pltpu.VMEM((TOGETHER * rows, 2 * width), f32),
            pltpu.VMEM((deep, 2, rows, width), bf16),
            pltpu.VMEM((deep, rows, width), bf16),
            pltpu.VMEM((deep - 1, rows, width), bf16),
            pltpu.VMEM((deep, rows, width), bf16),
            dma((deep - 1,)),
            dma((deep,)),
            dma((deep,)),
            dma((deep,)),
            dma((n - 1,)),
            dma((n - 1,)),
        ],
        compiler_params=pltpu.CompilerParams(collective_id=2, has_side_effects=True, vmem_limit_bytes=GRANT),
        cost_estimate=COST,
    )(rest, resid, x2, high, margin, owner, rank, loss_part)

    owned, gradient, loss = pl.pallas_call(
        finish_kernel,
        out_shape=(shape((1, ex), f32), shape((rows, width), f32), shape((1, 1), f32)),
        in_specs=[VM, VM],
        out_specs=(VM, VM, SM),
        compiler_params=pltpu.CompilerParams(vmem_limit_bytes=GRANT),
        cost_estimate=COST,
    )(total, notes)
    return owned.reshape(ex), gradient, loss.reshape(())


def solution(mesh):
    in_specs = (
        P("rows", "feat", None),
        P("rows", "feat"),
        P("rows", "feat"),
        P("rows"),
        P("rows"),
        P(("feat", "rows"), None),
    )
    out_specs = (P("rows"), P(("feat", "rows"), None), P())
    body = functools.partial(on_device, mesh.shape["rows"], mesh.shape["feat"])
    return jax.shard_map(body, mesh=mesh, in_specs=in_specs, out_specs=out_specs, check_vma=False)
```

```python
import functools

import jax
import jax.numpy as jnp
from jax import lax
from jax.experimental import pallas as pl
from jax.experimental.pallas import tpu as pltpu
from jax.sharding import PartitionSpec as P

MESH = pl.DeviceIdType.MESH
LANES = 128
GRAIN = 16
GROUP = 32
GRANT = 24 * 1024 * 1024
COST = pl.CostEstimate(flops=0, bytes_accessed=24 * 1024 * 1024, transcendentals=0)
NT = (((1,), (1,)), ((), ()))
NN = (((1,), (0,)), ((), ()))
VM = pl.BlockSpec(memory_space=pltpu.VMEM)
SM = pl.BlockSpec(memory_space=pltpu.SMEM)
ANY = pl.BlockSpec(memory_space=pltpu.HBM)
WIDE = GROUP * GRAIN
PER = LANES // GRAIN
CUT = 512
BATCH = 7
TOGETHER = 2


def seat(n):
    me = lax.axis_index("rows")
    side = lax.rem(me, 2)
    spot = me // 2
    partner = me + 1 - 2 * side
    deep = n // 2

    def listed(key):
        tables = [sorted((z for z in range(deep) if z != at), key=functools.partial(key, at)) for at in range(deep)]
        out = []
        for j in range(deep - 1):
            pick = tables[0][j]
            for at in range(1, deep):
                pick = pick + (tables[at][j] - tables[at - 1][j]) * ((spot + deep - at) // deep)
            out.append(pick)
        return out

    far = listed(lambda at, z: -abs(z - at))
    first = listed(lambda at, z: (abs(z - at)!=1, -abs(z - at)))
    return me, side, spot, partner, far, first


def call_out(axis, peers):
    barrier = pltpu.get_barrier_semaphore()
    for peer in peers:
        pl.semaphore_signal(barrier, inc=1, device_id={axis: peer}, device_id_type=MESH)
    return lambda: pl.semaphore_wait(barrier, len(peers))


def copy_to(axis, peer, source, target, send, recv):
    return pltpu.make_async_remote_copy(
        src_ref=source,
        dst_ref=target,
        send_sem=send,
        recv_sem=recv,
        device_id={axis: peer},
        device_id_type=MESH,
    )


def send_to(*args):
    copy = copy_to(*args)
    copy.start()
    return copy


def lane_group():
    return lax.broadcasted_iota(jnp.int32, (1, LANES), 1) // GRAIN


def own_lanes():
    sub = lax.broadcasted_iota(jnp.int32, (8, LANES), 0)
    return sub == lax.broadcasted_iota(jnp.int32, (8, LANES), 1) // GRAIN


def offsets(row):
    return jnp.broadcast_to(row, (8, WIDE)) - lax.broadcasted_iota(jnp.int32, (8, WIDE), 0)


def select_scores(pair, x2, offset, first, found):
    scores = lax.dot_general(pair, x2, NN, preferred_element_type=jnp.float32)
    for i in range(pair.shape[0] // 8):
        found = jnp.where(offset == first + i * 8, scores[i * 8 : i * 8 + 8, :], found)
    return found


def spread_sum(x2, offset, factor, firsts, rows):
    spread = jnp.concatenate(
        [jnp.where(offset == first + i * 8, factor, 0.0) for first in firsts for i in range(rows // 8)], axis=0
    ).astype(jnp.bfloat16)
    return lax.dot_general(spread, x2, NT, preferred_element_type=jnp.float32)


def put(x2_ref, hi_ref, t, values, id_row, rows):
    tall = x2_ref.shape[1] // 2
    chunk = id_row // rows
    odd = lax.rem(chunk, 2)
    hi_ref[t] = jnp.where(id_row < 0, -1, (chunk // 2) * rows + lax.rem(id_row, rows))
    odd = jnp.broadcast_to(odd.astype(jnp.float32), (16, WIDE))
    odd_half = jnp.concatenate([odd.astype(jnp.bfloat16)] * (tall // 16), axis=0)
    even_half = jnp.concatenate([(1.0 - odd).astype(jnp.bfloat16)] * (tall // 16), axis=0)
    flipped = values.T
    x2_ref[t, 0:tall, :] = flipped * even_half
    x2_ref[t, tall:, :] = flipped * odd_half


def listed_tiles(vals, idt, lists, t):
    hold = lists.shape[0] // 3
    row = t * GROUP // LANES
    col = lax.rem(t * GROUP, LANES)
    group = lane_group()
    values = jnp.concatenate([vals[lists[row, col + i]] for i in range(GROUP)], axis=0)
    parts = []
    for h in range(GROUP // PER):
        line = idt[pl.ds(lists[hold + row, col + h * PER], 1), :]
        for i in range(1, PER):
            line = jnp.where(group == i, idt[pl.ds(lists[hold + row, col + h * PER + i], 1), :], line)
        parts.append(line)
    return values, jnp.concatenate(parts, axis=1)


def gather_kernel(
    n, w_hbm, ids_hbm, used_hbm, owner_hbm, vals_hbm,
    table_ref, x2_ref, hi_ref, lists_ref, rank_ref, owner_ref, first_ref, rest_ref, vals, idt,
    w_buf, half, ids, used, own, lists, glist, found,
    send, recv, xsend, xrecv, here,
):
    local = [
        pltpu.make_async_copy(w_hbm, w_buf, here.at[0]),
        pltpu.make_async_copy(used_hbm, used, here.at[1]),
        pltpu.make_async_copy(ids_hbm, ids, here.at[2]),
        pltpu.make_async_copy(owner_hbm, own, here.at[3]),
        pltpu.make_async_copy(vals_hbm, vals, here.at[4]),
    ]
    for copy in local:
        copy.start()
    me, side, spot, partner, far, first = seat(n)
    deep = n // 2
    rows = w_buf.shape[0]
    slots, ex = ids.shape
    grains = slots // GRAIN
    joined = call_out("rows", [partner] + [2 * z + side for z in far])
    local[0].wait()
    half[...] = w_buf[...].astype(jnp.bfloat16)
    joined()
    across = [send_to("rows", partner, half, table_ref.at[me], xsend.at[spot], xrecv.at[spot])]
    along = [
        send_to("rows", 2 * z + side, half, table_ref.at[me], send.at[j], recv.at[spot])
        for j, z in enumerate(first)
    ]
    table_ref[me] = w_buf[...].astype(jnp.bfloat16)

    f32 = jnp.float32
    local[1].wait()
    count = (used[...] + (GRAIN - 1)) // GRAIN - 1
    sizes = jnp.broadcast_to(count, (LANES, ex)).T
    down = lax.broadcasted_iota(jnp.int32, (ex, LANES), 0)
    ends = sizes
    step = 1
    while step < ex:
        ends = ends + jnp.where(down >= step, pltpu.roll(ends, step, 0), 0)
        step *= 2
    lane = lax.broadcasted_iota(jnp.int32, (1, LANES), 1)
    span = ex * (grains - 1) // LANES
    hold = lists.shape[0] // 3
    for b in range(span):
        place = lane + b * LANES
        past = ends <= place
        which = jnp.sum(jnp.where(past, 1, 0), axis=0, keepdims=True)
        begin = jnp.sum(jnp.where(past, sizes, 0), axis=0, keepdims=True)
        live = which < ex
        q = place - begin + 1
        lists[b : b + 1, :] = jnp.clip(jnp.where(live, which * grains + q, 0), 0, grains * ex - 1)
        lists[hold + b : hold + b + 1, :] = jnp.clip(jnp.where(live, which + q * ex, grains * ex), 0, grains * ex)
    turns = (ends[ex - 8 : ex, :] + (GROUP - 1)) // GROUP
    lists[2 * hold :, :] = jnp.broadcast_to(turns[7:8, :], (hold, LANES))
    to_list = pltpu.make_async_copy(lists, glist, here.at[5])
    to_list.start()
    to_next = pltpu.make_async_copy(lists, lists_ref, here.at[6])
    to_next.start()

    local[2].wait()
    live = lax.broadcasted_iota(jnp.int32, (slots, ex), 0) < used[...]
    shifted = jnp.where(live, ids[...] + 1, 0)
    if slots < LANES:
        shifted = jnp.concatenate([shifted, jnp.zeros((LANES - slots, ex), jnp.int32)], axis=0)
    shifted = shifted.T
    grain_of = lax.broadcasted_iota(jnp.int32, (ex, LANES), 1) // GRAIN
    for q in range(grains):
        piece = jnp.where(grain_of == q, shifted, 0)
        step = GRAIN
        while step < LANES:
            piece = piece + pltpu.roll(piece, step, 1)
            step *= 2
        idt[q * ex : (q + 1) * ex, :] = piece - 1
    idt[grains * ex :, :] = jnp.full((8, LANES), -1, jnp.int32)

    mine = own_lanes()
    steady = ex // GROUP

    def prepare_first(t, carry):
        at = t * GROUP
        values = jnp.concatenate([vals[(at + i) * grains] for i in range(GROUP)], axis=0)
        parts = [
            jnp.sum(jnp.where(mine, idt[pl.ds(at + h * PER, PER), :], 0), axis=0, keepdims=True)
            for h in range(GROUP // PER)
        ]
        put(x2_ref, hi_ref, t, values, jnp.concatenate(parts, axis=1), rows)
        found[t] = jnp.zeros((8, WIDE), f32)
        return carry

    def prepare_rest(t, carry):
        values, id_row = listed_tiles(vals, idt, glist, t)
        put(x2_ref, hi_ref, steady + t, values, id_row, rows)
        found[steady + t] = jnp.zeros((8, WIDE), f32)
        return carry

    def score(z):
        pair = jnp.concatenate([table_ref[2 * z], table_ref[2 * z + 1]], axis=1)

        def turn(t, carry):
            found[t] = select_scores(pair, x2_ref[t], offsets(hi_ref[t]), z * rows, found[t])
            return carry

        lax.fori_loop(0, x2_ref.shape[0], turn, jnp.int32(0), unroll=True)

    local[4].wait()
    lax.fori_loop(0, steady, prepare_first, jnp.int32(0), unroll=2)
    to_list.wait()
    to_next.wait()

    def arrival(z):
        return copy_to("rows", partner, half, table_ref.at[2 * z + side], send.at[0], recv.at[z])

    def crossing(z):
        return copy_to("rows", partner, half, table_ref.at[2 * z + 1 - side], send.at[0], xrecv.at[z])

    near = far[::-1]
    lax.fori_loop(0, x2_ref.shape[0] - steady, prepare_rest, jnp.int32(0), unroll=2)
    for j, z in enumerate(near):
        arrival(z).wait_recv()
        block = table_ref.at[2 * z + side]
        across.append(send_to("rows", partner, block, block, xsend.at[z], xrecv.at[z]))
        if j == 0:
            crossing(spot).wait_recv()
            score(spot)

    local[3].wait()
    owner = own[...].astype(f32)
    square = jnp.broadcast_to(owner, (ex, ex))
    earlier = lax.broadcasted_iota(jnp.int32, (ex, ex), 0) < lax.broadcasted_iota(jnp.int32, (ex, ex), 1)
    same = jnp.where(jnp.logical_and(square.T == square, earlier), 1.0, 0.0)
    shift = lax.rem(me * (ex // n), LANES).astype(f32)
    rank = jnp.sum(same, axis=0, keepdims=True) + shift
    places = lax.broadcasted_iota(jnp.int32, (LANES, ex), 0).astype(f32)
    rank_ref[...] = jnp.where(places == rank, 1.0, 0.0)
    owner_ref[...] = jnp.broadcast_to(owner, owner_ref.shape)

    for z in near:
        crossing(z).wait_recv()
        score(z)
    for t in range(steady):
        term = jnp.sum(found[t], axis=0, keepdims=True)
        for h in range(GROUP // PER):
            at = t * GROUP + h * PER
            first_ref[at : at + PER, :] = jnp.where(mine, term[:, h * LANES : (h + 1) * LANES], 0.0)
    for t in range(x2_ref.shape[0] - steady):
        rest_ref[t] = jnp.sum(found[steady + t], axis=0, keepdims=True)
    for copy in along:
        copy.wait_send()
    for copy in across:
        copy.wait_send()


def margin_kernel(
    lists, table_ref, first_ref, rest_ref, vals, idt, partial_ref, more_x2, more_hi, terms
):
    n, rows, _ = table_ref.shape
    ex = partial_ref.shape[1]
    grains = terms.shape[0] // ex
    hold = lists.shape[0] // 3
    ready = rest_ref.shape[0]
    terms[ex:, :] = jnp.zeros((terms.shape[0] - ex, LANES), jnp.float32)
    group = lane_group()

    def one(x2, row):
        offset = offsets(row)
        found = jnp.zeros((8, WIDE), jnp.float32)
        for k in range(n // 2):
            pair = jnp.concatenate([table_ref[2 * k], table_ref[2 * k + 1]], axis=1)
            found = select_scores(pair, x2, offset, k * rows, found)
        return jnp.sum(found, axis=0, keepdims=True)

    def keep(t, term):
        row = t * GROUP // LANES
        col = lax.rem(t * GROUP, LANES)
        for i in range(GROUP):
            h = i // PER
            mine = jnp.where(group == i % PER, term[:, h * LANES : (h + 1) * LANES], 0.0)
            terms[pl.ds(lists[hold + row, col + i], 1), :] = mine

    def turn(t, carry):
        keep(t, rest_ref[t])
        return carry

    def late_turn(t, carry):
        values, id_row = listed_tiles(vals, idt, lists, t)
        put(more_x2, more_hi, t - ready, values, id_row, rows)
        keep(t, one(more_x2[t - ready], more_hi[t - ready]))
        return carry

    turns = lists[2 * hold, 0]
    lax.fori_loop(0, jnp.minimum(turns, ready), turn, jnp.int32(0))
    lax.fori_loop(ready, turns, late_turn, jnp.int32(0))
    spread = first_ref[...]
    for q in range(1, grains):
        spread = spread + terms[q * ex : (q + 1) * ex, :]
    partial_ref[...] = jnp.broadcast_to(jnp.sum(spread.T, axis=0, keepdims=True), partial_ref.shape)


def residual_kernel(n, partial_ref, labels_ref, margin_ref, resid_ref, loss_ref, held, send, recv):
    me = lax.axis_index("feat")
    peers = [lax.rem(me + k, n) for k in range(1, n)]
    call_out("feat", peers)()
    copies = [
        send_to("feat", peer, partial_ref, held.at[me], send.at[k], recv.at[k])
        for k, peer in enumerate(peers)
    ]
    held[me] = partial_ref[...]
    for copy in copies:
        copy.wait()
    margin = held[0]
    for k in range(1, n):
        margin = margin + held[k]
    label = labels_ref[...].astype(jnp.float32)
    residual = 1.0 / (1.0 + jnp.exp(-margin)) - label
    margin_ref[...] = margin
    resid_ref[...] = residual.astype(jnp.bfloat16).astype(jnp.float32)[0:1, :]
    term = jnp.maximum(margin, 0.0) + jnp.log1p(jnp.exp(-jnp.abs(margin))) - label * margin
    total = term[:, 0:LANES]
    for h in range(1, term.shape[1] // LANES):
        total = total + term[:, h * LANES : (h + 1) * LANES]
    loss_ref[...] = total


def factor_row(grains, lists, resid, t):
    group = lane_group()
    row_at = t * GROUP // LANES
    col = lax.rem(t * GROUP, LANES)
    parts = []
    for h in range(GROUP // PER):
        row = jnp.zeros((1, LANES), jnp.float32)
        for i in range(PER):
            row = jnp.where(group == i, resid[0, lists[row_at, col + h * PER + i] // grains], row)
        parts.append(row)
    return jnp.concatenate(parts, axis=1)


def late_kernel(grains, ready, lists, resid, more_x2, more_hi, total):
    turns = lists[lists.shape[0] // 3 * 2, 0]

    def turn(t, carry):
        factor = jnp.broadcast_to(factor_row(grains, lists, resid, t), (8, WIDE))
        x2, offset = more_x2[t - ready], offsets(more_hi[t - ready])
        for k in range(0, total.shape[0], CUT):
            total[k : k + CUT, :] += spread_sum(x2, offset, factor, [k], CUT)
        return carry

    @pl.when(turns > ready)
    def _():
        total[...] = jnp.zeros_like(total)
        lax.fori_loop(ready, turns, turn, jnp.int32(0))


def scatter_kernel(
    n, grains, lists_ref, rest_ref, resid_ref, x2_ref, hi_ref, margin_ref, owner_ref, rank_ref, loss_ref,
    sum_ref, notes_ref,
    lists, resid, here, notes, factors, acc, part, crossed, paired, held, send, recv, xsend, xrecv, nsend, nrecv,
):
    ex = margin_ref.shape[1]
    me, side, spot, partner, far, first = seat(n)
    deep = n // 2
    rows, width = sum_ref.shape
    others = [lax.rem(me + k, n) for k in range(1, n)]
    joined = call_out("rows", others)
    local = [
        pltpu.make_async_copy(lists_ref, lists, here.at[0]),
        pltpu.make_async_copy(resid_ref, resid, here.at[1]),
    ]
    for copy in local:
        copy.start()
    mine = own_lanes()
    steady = ex // GROUP
    ready = x2_ref.shape[0] - steady
    hold = lists.shape[0] // 3
    tall = jnp.broadcast_to(resid_ref[...], (LANES, ex)).T
    for t in range(steady):
        parts = [
            jnp.sum(
                jnp.where(mine, tall[t * GROUP + h * PER : t * GROUP + (h + 1) * PER, :], 0.0), axis=0, keepdims=True
            )
            for h in range(GROUP // PER)
        ]
        factors[t] = jnp.concatenate(parts, axis=1)
    for copy in local:
        copy.wait()

    def listed_factor(t, carry):
        factors[steady + t] = factor_row(grains, lists, resid, t)
        return carry

    lax.fori_loop(0, ready, listed_factor, jnp.int32(0), unroll=2)
    late = jnp.broadcast_to(lists_ref[2 * hold : 2 * hold + 1, 0:1] > ready, (rows, 2 * width))

    batch = max(b for b in range(1, BATCH + 1) if (steady + ready) % b == 0)

    def gather_pairs(js, zs):
        for i, z in enumerate(zs):
            more = rest_ref[pl.ds(pl.multiple_of(z * rows, rows), rows), :]
            acc[i * rows : (i + 1) * rows, :] = jnp.where(late, more, 0.0)
        high = len(js) * rows

        def turn(step, carry):
            part_sum = None
            for i in range(batch):
                t = step * batch + i
                factor = jnp.broadcast_to(factors[t], (8, WIDE))
                more = spread_sum(x2_ref[t], offsets(hi_ref[t]), factor, [z * rows for z in zs], rows)
                part_sum = more if part_sum is None else part_sum + more
            acc[0:high, :] += part_sum
            return carry

        lax.fori_loop(0, (steady + ready) // batch, turn, jnp.int32(0))
        for i, j in enumerate(js):
            part[j, 0] = acc[i * rows : (i + 1) * rows, 0:width].astype(jnp.bfloat16)
            part[j, 1] = acc[i * rows : (i + 1) * rows, width:].astype(jnp.bfloat16)

    def cross(j):
        return send_to("rows", partner, part.at[j, 1 - side], crossed.at[j], xsend.at[j], xrecv.at[j])

    across = []
    along = []

    def pass_on(j):
        across[j].wait_recv()
        pair = part[j, side].astype(jnp.float32) + crossed[j].astype(jnp.float32)
        paired[j] = pair.astype(jnp.bfloat16)
        along.append(
            send_to("rows", 2 * far[j] + side, paired.at[j], held.at[spot], send.at[j], recv.at[spot])
        )

    last = deep - 1
    planes = far + [spot]
    for j in range(0, deep, TOGETHER):
        js = list(range(j, min(j + TOGETHER, deep)))
        gather_pairs(js, [planes[i] for i in js])
        if j == 0:
            joined()
        across += [cross(i) for i in js]

    which = lax.broadcasted_iota(jnp.int32, (n, ex), 0).astype(jnp.float32)
    by_owner = jnp.where(which == owner_ref[0:1, :], margin_ref[0:1, :], 0.0)
    ordered = lax.dot_general(
        by_owner, rank_ref[...], NT, precision=lax.Precision.HIGHEST, preferred_element_type=jnp.float32
    )
    sub = lax.broadcasted_iota(jnp.int32, (8, LANES), 0)
    for d in range(n):
        notes[d] = jnp.where(sub == 0, ordered[d : d + 1, :], loss_ref[...])
    told = [
        send_to("rows", peer, notes.at[peer], notes_ref.at[me], nsend.at[k], nrecv.at[k])
        for k, peer in enumerate(others)
    ]
    notes_ref[me] = notes[me]
    for j in range(last):
        pass_on(j)
    across[last].wait_recv()
    total = part[last, side].astype(jnp.float32) + crossed[last].astype(jnp.float32)
    for z in far[::-1]:
        copy_to("rows", partner, paired.at[0], held.at[z], send.at[0], recv.at[z]).wait_recv()
        total = total + held[z].astype(jnp.float32)
    sum_ref[...] = total
    for copy in across:
        copy.wait_send()
    for copy in along:
        copy.wait_send()
    for copy in told:
        copy.wait()


def finish_kernel(sum_ref, notes_ref, owned_ref, grad_ref, loss_ref):
    n = notes_ref.shape[0]
    ex = owned_ref.shape[1]
    grad_ref[...] = sum_ref[...]
    for h in range(ex // LANES):
        row = jnp.zeros((1, LANES), jnp.float32)
        for d in range(n):
            if d * (ex // n) // LANES == h:
                row = row + notes_ref[d, 0:1, :]
        owned_ref[:, h * LANES : (h + 1) * LANES] = row
    loss = jnp.zeros((1, LANES), jnp.float32)
    for d in range(n):
        loss = loss + notes_ref[d, 1:2, :]
    loss_ref[0, 0] = jnp.sum(loss) * (1.0 / (ex * n))


def on_device(n, nf, tile_values, tile_blocks, tile_counts, labels, owner_rank, weights):
    ex, slots, width = tile_values.shape
    grains = slots // GRAIN
    rows = weights.shape[0]
    deep = n // 2
    steady = ex // GROUP
    ready = min(6, (grains - 1) * steady)
    late = max((grains - 1) * steady - ready, 1)
    hold = -(-(ex * (grains - 1)) // (8 * LANES)) * 8
    f32, i32, bf16 = jnp.float32, jnp.int32, jnp.bfloat16
    shape = jax.ShapeDtypeStruct
    dma = pltpu.SemaphoreType.DMA
    vals = tile_values.reshape(ex * grains, GRAIN, width)

    table, x2, high, lists, rank, owner, first, found, packed, named = pl.pallas_call(
        functools.partial(gather_kernel, n),
        out_shape=(
            shape((n, rows, width), bf16),
            shape((steady + ready, 2 * width, WIDE), bf16),
            shape((steady + ready, 1, WIDE), i32),
            shape((3 * hold, LANES), i32),
            shape((LANES, ex), f32),
            shape((8, ex), f32),
            shape((ex, LANES), f32),
            shape((ready, 1, WIDE), f32),
            shape((ex * grains, GRAIN, width), bf16),
            shape((ex * grains + 8, LANES), i32),
        ),
        in_specs=[ANY] * 5,
        out_specs=(VM, VM, VM, SM, VM, VM, VM, VM, VM, VM),
        scratch_shapes=[
            pltpu.VMEM((rows, width), f32),
            pltpu.VMEM((rows, width), bf16),
            pltpu.VMEM((slots, ex), i32),
            pltpu.VMEM((1, ex), i32),
            pltpu.VMEM((1, ex), i32),
            pltpu.VMEM((3 * hold, LANES), i32),
            pltpu.SMEM((3 * hold, LANES), i32),
            pltpu.VMEM((steady + ready, 8, WIDE), f32),
            dma((deep - 1,)), dma((deep,)), dma((deep,)), dma((deep,)), dma((7,)),
        ],
        compiler_params=pltpu.CompilerParams(collective_id=0, has_side_effects=True, vmem_limit_bytes=GRANT),
        cost_estimate=COST,
    )(*[
        pltpu.with_memory_space_constraint(a, pltpu.HBM)
        for a in (weights, tile_blocks.T, tile_counts.reshape(1, ex), owner_rank.reshape(1, ex), vals)
    ])

    partial, more_x2, more_high = pl.pallas_call(
        margin_kernel,
        out_shape=(shape((8, ex), f32), shape((late, 2 * width, WIDE), bf16), shape((late, 1, WIDE), i32)),
        in_specs=[SM] + [VM] * 5,
        out_specs=(VM, VM, VM),
        scratch_shapes=[pltpu.VMEM((ex * grains + 8, LANES), f32)],
        compiler_params=pltpu.CompilerParams(vmem_limit_bytes=GRANT),
        cost_estimate=COST,
    )(lists, table, first, found, packed, named)

    margin, resid, loss_part = pl.pallas_call(
        functools.partial(residual_kernel, nf),
        out_shape=(shape((8, ex), f32), shape((1, ex), f32), shape((8, LANES), f32)),
        in_specs=[VM, VM],
        out_specs=(VM, VM, VM),
        scratch_shapes=[pltpu.VMEM((nf, 8, ex), f32), dma((nf - 1,)), dma((nf - 1,))],
        compiler_params=pltpu.CompilerParams(collective_id=1, has_side_effects=True, vmem_limit_bytes=GRANT),
        cost_estimate=COST,
    )(partial, labels.reshape(1, ex))

    rest = pl.pallas_call(
        functools.partial(late_kernel, grains, ready),
        out_shape=shape((deep * rows, 2 * width), f32),
        in_specs=[SM, SM, VM, VM],
        out_specs=VM,
        compiler_params=pltpu.CompilerParams(vmem_limit_bytes=GRANT),
        cost_estimate=COST,
    )(lists, resid, more_x2, more_high)

    total, notes = pl.pallas_call(
        functools.partial(scatter_kernel, n, grains),
        out_shape=(shape((rows, width), f32), shape((n, 8, LANES), f32)),
        in_specs=[VM] * 9,
        out_specs=(VM, VM),
        scratch_shapes=[
            pltpu.SMEM((3 * hold, LANES), i32),
            pltpu.SMEM((1, ex), f32),
            dma((2,)),
            pltpu.VMEM((n, 8, LANES), f32),
            pltpu.VMEM((steady + ready, 1, WIDE), f32),
            pltpu.VMEM((TOGETHER * rows, 2 * width), f32),
            pltpu.VMEM((deep, 2, rows, width), bf16),
            pltpu.VMEM((deep, rows, width), bf16),
            pltpu.VMEM((deep - 1, rows, width), bf16),
            pltpu.VMEM((deep, rows, width), bf16),
            dma((deep - 1,)),
            dma((deep,)),
            dma((deep,)),
            dma((deep,)),
            dma((n - 1,)),
            dma((n - 1,)),
        ],
        compiler_params=pltpu.CompilerParams(collective_id=2, has_side_effects=True, vmem_limit_bytes=GRANT),
        cost_estimate=COST,
    )(lists, rest, resid, x2, high, margin, owner, rank, loss_part)

    owned, gradient, loss = pl.pallas_call(
        finish_kernel,
        out_shape=(shape((1, ex), f32), shape((rows, width), f32), shape((1, 1), f32)),
        in_specs=[VM, VM],
        out_specs=(VM, VM, SM),
        compiler_params=pltpu.CompilerParams(vmem_limit_bytes=GRANT),
        cost_estimate=COST,
    )(total, notes)
    return owned.reshape(ex), gradient, loss.reshape(())


def solution(mesh):
    in_specs = (
        P("rows", "feat", None),
        P("rows", "feat"),
        P("rows", "feat"),
        P("rows"),
        P("rows"),
        P(("feat", "rows"), None),
    )
    out_specs = (P("rows"), P(("feat", "rows"), None), P())
    body = functools.partial(on_device, mesh.shape["rows"], mesh.shape["feat"])
    return jax.shard_map(body, mesh=mesh, in_specs=in_specs, out_specs=out_specs, check_vma=False)
```

```python
import functools

import jax
import jax.numpy as jnp
from jax import lax
from jax.experimental import pallas as pl
from jax.experimental.pallas import tpu as pltpu
from jax.sharding import PartitionSpec as P

MESH = pl.DeviceIdType.MESH
LANES = 128
GRAIN = 16
GROUP = 32
GRANT = 24 * 1024 * 1024
COST = pl.CostEstimate(flops=0, bytes_accessed=24 * 1024 * 1024, transcendentals=0)
NT = (((1,), (1,)), ((), ()))
NN = (((1,), (0,)), ((), ()))
VM = pl.BlockSpec(memory_space=pltpu.VMEM)
SM = pl.BlockSpec(memory_space=pltpu.SMEM)
ANY = pl.BlockSpec(memory_space=pltpu.HBM)
WIDE = GROUP * GRAIN
PER = LANES // GRAIN
CUT = 512
BATCH = 7
TOGETHER = 2


def seat(n):
    me = lax.axis_index("rows")
    side = lax.rem(me, 2)
    spot = me // 2
    partner = me + 1 - 2 * side
    deep = n // 2

    def listed(key):
        tables = [sorted((z for z in range(deep) if z != at), key=functools.partial(key, at)) for at in range(deep)]
        out = []
        for j in range(deep - 1):
            pick = tables[0][j]
            for at in range(1, deep):
                pick = pick + (tables[at][j] - tables[at - 1][j]) * ((spot + deep - at) // deep)
            out.append(pick)
        return out

    far = listed(lambda at, z: -abs(z - at))
    first = listed(lambda at, z: (abs(z - at)!=1, -abs(z - at)))
    return me, side, spot, partner, far, first


def call_out(axis, peers):
    barrier = pltpu.get_barrier_semaphore()
    for peer in peers:
        pl.semaphore_signal(barrier, inc=1, device_id={axis: peer}, device_id_type=MESH)
    return lambda: pl.semaphore_wait(barrier, len(peers))


def copy_to(axis, peer, source, target, send, recv):
    return pltpu.make_async_remote_copy(
        src_ref=source,
        dst_ref=target,
        send_sem=send,
        recv_sem=recv,
        device_id={axis: peer},
        device_id_type=MESH,
    )


def send_to(*args):
    copy = copy_to(*args)
    copy.start()
    return copy


def lane_group():
    return lax.broadcasted_iota(jnp.int32, (1, LANES), 1) // GRAIN


def own_lanes():
    sub = lax.broadcasted_iota(jnp.int32, (8, LANES), 0)
    return sub == lax.broadcasted_iota(jnp.int32, (8, LANES), 1) // GRAIN


def offsets(row):
    return jnp.broadcast_to(row, (8, WIDE)) - lax.broadcasted_iota(jnp.int32, (8, WIDE), 0)


def select_scores(pair, x2, offset, first, found):
    scores = lax.dot_general(pair, x2, NN, preferred_element_type=jnp.float32)
    for i in range(pair.shape[0] // 8):
        found = jnp.where(offset == first + i * 8, scores[i * 8 : i * 8 + 8, :], found)
    return found


def spread_sum(x2, offset, factor, firsts, rows):
    spread = jnp.concatenate(
        [jnp.where(offset == first + i * 8, factor, 0.0) for first in firsts for i in range(rows // 8)], axis=0
    ).astype(jnp.bfloat16)
    return lax.dot_general(spread, x2, NT, preferred_element_type=jnp.float32)


def put(x2_ref, hi_ref, t, values, id_row, rows):
    tall = x2_ref.shape[1] // 2
    chunk = id_row // rows
    odd = lax.rem(chunk, 2)
    hi_ref[t] = jnp.where(id_row < 0, -1, (chunk // 2) * rows + lax.rem(id_row, rows))
    odd = jnp.broadcast_to(odd.astype(jnp.float32), (16, WIDE))
    odd_half = jnp.concatenate([odd.astype(jnp.bfloat16)] * (tall // 16), axis=0)
    even_half = jnp.concatenate([(1.0 - odd).astype(jnp.bfloat16)] * (tall // 16), axis=0)
    flipped = values.T
    x2_ref[t, 0:tall, :] = flipped * even_half
    x2_ref[t, tall:, :] = flipped * odd_half


def listed_tiles(vals, idt, lists, t):
    hold = lists.shape[0] // 3
    row = t * GROUP // LANES
    col = lax.rem(t * GROUP, LANES)
    group = lane_group()
    values = jnp.concatenate([vals[lists[row, col + i]] for i in range(GROUP)], axis=0)
    parts = []
    for h in range(GROUP // PER):
        line = idt[pl.ds(lists[hold + row, col + h * PER], 1), :]
        for i in range(1, PER):
            line = jnp.where(group == i, idt[pl.ds(lists[hold + row, col + h * PER + i], 1), :], line)
        parts.append(line)
    return values, jnp.concatenate(parts, axis=1)


def gather_kernel(
    n, w_hbm, ids_hbm, used_hbm, owner_hbm, vals_hbm,
    table_ref, x2_ref, hi_ref, lists_ref, rank_ref, owner_ref, first_ref, rest_ref, vals, idt,
    w_buf, half, ids, used, own, lists, glist, found,
    send, recv, xsend, xrecv, here,
):
    local = [
        pltpu.make_async_copy(w_hbm, w_buf, here.at[0]),
        pltpu.make_async_copy(used_hbm, used, here.at[1]),
        pltpu.make_async_copy(ids_hbm, ids, here.at[2]),
        pltpu.make_async_copy(owner_hbm, own, here.at[3]),
        pltpu.make_async_copy(vals_hbm, vals, here.at[4]),
    ]
    for copy in local:
        copy.start()
    me, side, spot, partner, far, first = seat(n)
    deep = n // 2
    rows = w_buf.shape[0]
    slots, ex = ids.shape
    grains = slots // GRAIN
    joined = call_out("rows", [partner] + [2 * z + side for z in far])
    local[0].wait()
    half[...] = w_buf[...].astype(jnp.bfloat16)
    joined()
    across = [send_to("rows", partner, half, table_ref.at[me], xsend.at[spot], xrecv.at[spot])]
    along = [
        send_to("rows", 2 * z + side, half, table_ref.at[me], send.at[j], recv.at[spot])
        for j, z in enumerate(first)
    ]
    table_ref[me] = w_buf[...].astype(jnp.bfloat16)

    f32 = jnp.float32
    local[1].wait()
    count = (used[...] + (GRAIN - 1)) // GRAIN - 1
    sizes = jnp.broadcast_to(count, (LANES, ex)).T
    down = lax.broadcasted_iota(jnp.int32, (ex, LANES), 0)
    ends = sizes
    step = 1
    while step < ex:
        ends = ends + jnp.where(down >= step, pltpu.roll(ends, step, 0), 0)
        step *= 2
    lane = lax.broadcasted_iota(jnp.int32, (1, LANES), 1)
    span = ex * (grains - 1) // LANES
    hold = lists.shape[0] // 3
    for b in range(span):
        place = lane + b * LANES
        past = ends <= place
        which = jnp.sum(jnp.where(past, 1, 0), axis=0, keepdims=True)
        begin = jnp.sum(jnp.where(past, sizes, 0), axis=0, keepdims=True)
        live = which < ex
        q = place - begin + 1
        lists[b : b + 1, :] = jnp.clip(jnp.where(live, which * grains + q, 0), 0, grains * ex - 1)
        lists[hold + b : hold + b + 1, :] = jnp.clip(jnp.where(live, which + q * ex, grains * ex), 0, grains * ex)
    turns = (ends[ex - 8 : ex, :] + (GROUP - 1)) // GROUP
    lists[2 * hold :, :] = jnp.broadcast_to(turns[7:8, :], (hold, LANES))
    to_list = pltpu.make_async_copy(lists, glist, here.at[5])
    to_list.start()
    to_next = pltpu.make_async_copy(lists, lists_ref, here.at[6])
    to_next.start()

    local[2].wait()
    live = lax.broadcasted_iota(jnp.int32, (slots, ex), 0) < used[...]
    shifted = jnp.where(live, ids[...] + 1, 0)
    if slots < LANES:
        shifted = jnp.concatenate([shifted, jnp.zeros((LANES - slots, ex), jnp.int32)], axis=0)
    shifted = shifted.T
    grain_of = lax.broadcasted_iota(jnp.int32, (ex, LANES), 1) // GRAIN
    for q in range(grains):
        piece = jnp.where(grain_of == q, shifted, 0)
        step = GRAIN
        while step < LANES:
            piece = piece + pltpu.roll(piece, step, 1)
            step *= 2
        idt[q * ex : (q + 1) * ex, :] = piece - 1
    idt[grains * ex :, :] = jnp.full((8, LANES), -1, jnp.int32)

    mine = own_lanes()
    steady = ex // GROUP

    def prepare_first(t, carry):
        at = t * GROUP
        values = jnp.concatenate([vals[(at + i) * grains] for i in range(GROUP)], axis=0)
        parts = [
            jnp.sum(jnp.where(mine, idt[pl.ds(at + h * PER, PER), :], 0), axis=0, keepdims=True)
            for h in range(GROUP // PER)
        ]
        put(x2_ref, hi_ref, t, values, jnp.concatenate(parts, axis=1), rows)
        found[t] = jnp.zeros((8, WIDE), f32)
        return carry

    def prepare_rest(t, carry):
        values, id_row = listed_tiles(vals, idt, glist, t)
        put(x2_ref, hi_ref, steady + t, values, id_row, rows)
        found[steady + t] = jnp.zeros((8, WIDE), f32)
        return carry

    def score(z):
        pair = jnp.concatenate([table_ref[2 * z], table_ref[2 * z + 1]], axis=1)

        def turn(t, carry):
            found[t] = select_scores(pair, x2_ref[t], offsets(hi_ref[t]), z * rows, found[t])
            return carry

        lax.fori_loop(0, x2_ref.shape[0], turn, jnp.int32(0), unroll=True)

    local[4].wait()
    lax.fori_loop(0, steady, prepare_first, jnp.int32(0), unroll=2)
    to_list.wait()
    to_next.wait()

    def arrival(z):
        return copy_to("rows", partner, half, table_ref.at[2 * z + side], send.at[0], recv.at[z])

    def crossing(z):
        return copy_to("rows", partner, half, table_ref.at[2 * z + 1 - side], send.at[0], xrecv.at[z])

    near = far[::-1]
    lax.fori_loop(0, x2_ref.shape[0] - steady, prepare_rest, jnp.int32(0), unroll=2)
    for j, z in enumerate(near):
        arrival(z).wait_recv()
        block = table_ref.at[2 * z + side]
        across.append(send_to("rows", partner, block, block, xsend.at[z], xrecv.at[z]))
        if j == 0:
            crossing(spot).wait_recv()
            score(spot)

    local[3].wait()
    owner = own[...].astype(f32)
    square = jnp.broadcast_to(owner, (ex, ex))
    earlier = lax.broadcasted_iota(jnp.int32, (ex, ex), 0) < lax.broadcasted_iota(jnp.int32, (ex, ex), 1)
    same = jnp.where(jnp.logical_and(square.T == square, earlier), 1.0, 0.0)
    shift = lax.rem(me * (ex // n), LANES).astype(f32)
    rank = jnp.sum(same, axis=0, keepdims=True) + shift
    places = lax.broadcasted_iota(jnp.int32, (LANES, ex), 0).astype(f32)
    rank_ref[...] = jnp.where(places == rank, 1.0, 0.0)
    owner_ref[...] = jnp.broadcast_to(owner, owner_ref.shape)

    for z in near:
        crossing(z).wait_recv()
        score(z)
    for t in range(steady):
        term = jnp.sum(found[t], axis=0, keepdims=True)
        for h in range(GROUP // PER):
            at = t * GROUP + h * PER
            first_ref[at : at + PER, :] = jnp.where(mine, term[:, h * LANES : (h + 1) * LANES], 0.0)
    for t in range(x2_ref.shape[0] - steady):
        rest_ref[t] = jnp.sum(found[steady + t], axis=0, keepdims=True)
    for copy in along:
        copy.wait_send()
    for copy in across:
        copy.wait_send()


def margin_kernel(
    lists, table_ref, first_ref, rest_ref, vals, idt, partial_ref, more_x2, more_hi, terms
):
    n, rows, _ = table_ref.shape
    ex = partial_ref.shape[1]
    grains = terms.shape[0] // ex
    hold = lists.shape[0] // 3
    ready = rest_ref.shape[0]
    terms[ex:, :] = jnp.zeros((terms.shape[0] - ex, LANES), jnp.float32)
    group = lane_group()

    def one(x2, row):
        offset = offsets(row)
        found = jnp.zeros((8, WIDE), jnp.float32)
        for k in range(n // 2):
            pair = jnp.concatenate([table_ref[2 * k], table_ref[2 * k + 1]], axis=1)
            found = select_scores(pair, x2, offset, k * rows, found)
        return jnp.sum(found, axis=0, keepdims=True)

    def keep(t, term):
        row = t * GROUP // LANES
        col = lax.rem(t * GROUP, LANES)
        for i in range(GROUP):
            h = i // PER
            mine = jnp.where(group == i % PER, term[:, h * LANES : (h + 1) * LANES], 0.0)
            terms[pl.ds(lists[hold + row, col + i], 1), :] = mine

    def turn(t, carry):
        keep(t, rest_ref[t])
        return carry

    def late_turn(t, carry):
        values, id_row = listed_tiles(vals, idt, lists, t)
        put(more_x2, more_hi, t - ready, values, id_row, rows)
        keep(t, one(more_x2[t - ready], more_hi[t - ready]))
        return carry

    turns = lists[2 * hold, 0]
    lax.fori_loop(0, jnp.minimum(turns, ready), turn, jnp.int32(0))
    lax.fori_loop(ready, turns, late_turn, jnp.int32(0))
    spread = first_ref[...]
    for q in range(1, grains):
        spread = spread + terms[q * ex : (q + 1) * ex, :]
    partial_ref[...] = jnp.broadcast_to(jnp.sum(spread.T, axis=0, keepdims=True), partial_ref.shape)


def residual_kernel(n, partial_ref, labels_ref, margin_ref, resid_ref, loss_ref, held, send, recv):
    me = lax.axis_index("feat")
    peers = [lax.rem(me + k, n) for k in range(1, n)]
    call_out("feat", peers)()
    copies = [
        send_to("feat", peer, partial_ref, held.at[me], send.at[k], recv.at[k])
        for k, peer in enumerate(peers)
    ]
    held[me] = partial_ref[...]
    for copy in copies:
        copy.wait()
    margin = held[0]
    for k in range(1, n):
        margin = margin + held[k]
    label = labels_ref[...].astype(jnp.float32)
    residual = 1.0 / (1.0 + jnp.exp(-margin)) - label
    margin_ref[...] = margin
    resid_ref[...] = residual.astype(jnp.bfloat16).astype(jnp.float32)[0:1, :]
    term = jnp.maximum(margin, 0.0) + jnp.log1p(jnp.exp(-jnp.abs(margin))) - label * margin
    total = term[:, 0:LANES]
    for h in range(1, term.shape[1] // LANES):
        total = total + term[:, h * LANES : (h + 1) * LANES]
    loss_ref[...] = total


def factor_row(grains, lists, resid, t):
    group = lane_group()
    row_at = t * GROUP // LANES
    col = lax.rem(t * GROUP, LANES)
    parts = []
    for h in range(GROUP // PER):
        row = jnp.zeros((1, LANES), jnp.float32)
        for i in range(PER):
            row = jnp.where(group == i, resid[0, lists[row_at, col + h * PER + i] // grains], row)
        parts.append(row)
    return jnp.concatenate(parts, axis=1)


def late_kernel(grains, ready, lists_ref, resid_ref, more_x2, more_hi, total, lists, resid, here):
    hold = lists.shape[0] // 3

    def turn(t, carry):
        factor = jnp.broadcast_to(factor_row(grains, lists, resid, t), (8, WIDE))
        x2, offset = more_x2[t - ready], offsets(more_hi[t - ready])
        for k in range(0, total.shape[0], CUT):
            total[k : k + CUT, :] += spread_sum(x2, offset, factor, [k], CUT)
        return carry

    @pl.when(jnp.max(lists_ref[2 * hold :, :]) > ready)
    def _():
        copies = [
            pltpu.make_async_copy(lists_ref, lists, here.at[0]),
            pltpu.make_async_copy(resid_ref, resid, here.at[1]),
        ]
        for copy in copies:
            copy.start()
        total[...] = jnp.zeros_like(total)
        for copy in copies:
            copy.wait()
        lax.fori_loop(ready, lists[2 * hold, 0], turn, jnp.int32(0))


def scatter_kernel(
    n, grains, lists_ref, rest_ref, resid_ref, x2_ref, hi_ref, margin_ref, owner_ref, rank_ref, loss_ref,
    sum_ref, notes_ref,
    lists, resid, here, notes, factors, acc, part, crossed, paired, held, send, recv, xsend, xrecv, nsend, nrecv,
):
    ex = margin_ref.shape[1]
    me, side, spot, partner, far, first = seat(n)
    deep = n // 2
    rows, width = sum_ref.shape
    others = [lax.rem(me + k, n) for k in range(1, n)]
    joined = call_out("rows", others)
    local = [
        pltpu.make_async_copy(lists_ref, lists, here.at[0]),
        pltpu.make_async_copy(resid_ref, resid, here.at[1]),
    ]
    for copy in local:
        copy.start()
    mine = own_lanes()
    steady = ex // GROUP
    ready = x2_ref.shape[0] - steady
    hold = lists.shape[0] // 3
    tall = jnp.broadcast_to(resid_ref[...], (LANES, ex)).T
    for t in range(steady):
        parts = [
            jnp.sum(
                jnp.where(mine, tall[t * GROUP + h * PER : t * GROUP + (h + 1) * PER, :], 0.0), axis=0, keepdims=True
            )
            for h in range(GROUP // PER)
        ]
        factors[t] = jnp.concatenate(parts, axis=1)
    for copy in local:
        copy.wait()

    def listed_factor(t, carry):
        factors[steady + t] = factor_row(grains, lists, resid, t)
        return carry

    lax.fori_loop(0, ready, listed_factor, jnp.int32(0), unroll=2)
    late = jnp.broadcast_to(lists_ref[2 * hold : 2 * hold + 1, 0:1] > ready, (rows, 2 * width))

    batch = max(b for b in range(1, BATCH + 1) if (steady + ready) % b == 0)

    def gather_pairs(js, zs):
        for i, z in enumerate(zs):
            more = rest_ref[pl.ds(pl.multiple_of(z * rows, rows), rows), :]
            acc[i * rows : (i + 1) * rows, :] = jnp.where(late, more, 0.0)
        high = len(js) * rows

        def turn(step, carry):
            part_sum = None
            for i in range(batch):
                t = step * batch + i
                factor = jnp.broadcast_to(factors[t], (8, WIDE))
                more = spread_sum(x2_ref[t], offsets(hi_ref[t]), factor, [z * rows for z in zs], rows)
                part_sum = more if part_sum is None else part_sum + more
            acc[0:high, :] += part_sum
            return carry

        lax.fori_loop(0, (steady + ready) // batch, turn, jnp.int32(0))
        for i, j in enumerate(js):
            part[j, 0] = acc[i * rows : (i + 1) * rows, 0:width].astype(jnp.bfloat16)
            part[j, 1] = acc[i * rows : (i + 1) * rows, width:].astype(jnp.bfloat16)

    def cross(j):
        return send_to("rows", partner, part.at[j, 1 - side], crossed.at[j], xsend.at[j], xrecv.at[j])

    across = []
    along = []

    def pass_on(j):
        across[j].wait_recv()
        pair = part[j, side].astype(jnp.float32) + crossed[j].astype(jnp.float32)
        paired[j] = pair.astype(jnp.bfloat16)
        along.append(
            send_to("rows", 2 * far[j] + side, paired.at[j], held.at[spot], send.at[j], recv.at[spot])
        )

    last = deep - 1
    planes = far + [spot]
    for j in range(0, deep, TOGETHER):
        js = list(range(j, min(j + TOGETHER, deep)))
        gather_pairs(js, [planes[i] for i in js])
        if j == 0:
            joined()
        across += [cross(i) for i in js]

    which = lax.broadcasted_iota(jnp.int32, (n, ex), 0).astype(jnp.float32)
    by_owner = jnp.where(which == owner_ref[0:1, :], margin_ref[0:1, :], 0.0)
    ordered = lax.dot_general(
        by_owner, rank_ref[...], NT, precision=lax.Precision.HIGHEST, preferred_element_type=jnp.float32
    )
    sub = lax.broadcasted_iota(jnp.int32, (8, LANES), 0)
    for d in range(n):
        notes[d] = jnp.where(sub == 0, ordered[d : d + 1, :], loss_ref[...])
    told = [
        send_to("rows", peer, notes.at[peer], notes_ref.at[me], nsend.at[k], nrecv.at[k])
        for k, peer in enumerate(others)
    ]
    notes_ref[me] = notes[me]
    for j in range(last):
        pass_on(j)
    across[last].wait_recv()
    total = part[last, side].astype(jnp.float32) + crossed[last].astype(jnp.float32)
    for z in far[::-1]:
        copy_to("rows", partner, paired.at[0], held.at[z], send.at[0], recv.at[z]).wait_recv()
        total = total + held[z].astype(jnp.float32)
    sum_ref[...] = total
    for copy in across:
        copy.wait_send()
    for copy in along:
        copy.wait_send()
    for copy in told:
        copy.wait()


def finish_kernel(sum_ref, notes_ref, owned_ref, grad_ref, loss_ref):
    n = notes_ref.shape[0]
    ex = owned_ref.shape[1]
    grad_ref[...] = sum_ref[...]
    for h in range(ex // LANES):
        row = jnp.zeros((1, LANES), jnp.float32)
        for d in range(n):
            if d * (ex // n) // LANES == h:
                row = row + notes_ref[d, 0:1, :]
        owned_ref[:, h * LANES : (h + 1) * LANES] = row
    loss = jnp.zeros((1, LANES), jnp.float32)
    for d in range(n):
        loss = loss + notes_ref[d, 1:2, :]
    loss_ref[0, 0] = jnp.sum(loss) * (1.0 / (ex * n))


def on_device(n, nf, tile_values, tile_blocks, tile_counts, labels, owner_rank, weights):
    ex, slots, width = tile_values.shape
    grains = slots // GRAIN
    rows = weights.shape[0]
    deep = n // 2
    steady = ex // GROUP
    ready = min(6, (grains - 1) * steady)
    late = max((grains - 1) * steady - ready, 1)
    hold = -(-(ex * (grains - 1)) // (8 * LANES)) * 8
    f32, i32, bf16 = jnp.float32, jnp.int32, jnp.bfloat16
    shape = jax.ShapeDtypeStruct
    dma = pltpu.SemaphoreType.DMA
    vals = tile_values.reshape(ex * grains, GRAIN, width)

    table, x2, high, lists, rank, owner, first, found, packed, named = pl.pallas_call(
        functools.partial(gather_kernel, n),
        out_shape=(
            shape((n, rows, width), bf16),
            shape((steady + ready, 2 * width, WIDE), bf16),
            shape((steady + ready, 1, WIDE), i32),
            shape((3 * hold, LANES), i32),
            shape((LANES, ex), f32),
            shape((8, ex), f32),
            shape((ex, LANES), f32),
            shape((ready, 1, WIDE), f32),
            shape((ex * grains, GRAIN, width), bf16),
            shape((ex * grains + 8, LANES), i32),
        ),
        in_specs=[ANY] * 5,
        out_specs=(VM, VM, VM, SM, VM, VM, VM, VM, VM, VM),
        scratch_shapes=[
            pltpu.VMEM((rows, width), f32),
            pltpu.VMEM((rows, width), bf16),
            pltpu.VMEM((slots, ex), i32),
            pltpu.VMEM((1, ex), i32),
            pltpu.VMEM((1, ex), i32),
            pltpu.VMEM((3 * hold, LANES), i32),
            pltpu.SMEM((3 * hold, LANES), i32),
            pltpu.VMEM((steady + ready, 8, WIDE), f32),
            dma((deep - 1,)), dma((deep,)), dma((deep,)), dma((deep,)), dma((7,)),
        ],
        compiler_params=pltpu.CompilerParams(collective_id=0, has_side_effects=True, vmem_limit_bytes=GRANT),
        cost_estimate=COST,
    )(*[
        pltpu.with_memory_space_constraint(a, pltpu.HBM)
        for a in (weights, tile_blocks.T, tile_counts.reshape(1, ex), owner_rank.reshape(1, ex), vals)
    ])

    partial, more_x2, more_high = pl.pallas_call(
        margin_kernel,
        out_shape=(shape((8, ex), f32), shape((late, 2 * width, WIDE), bf16), shape((late, 1, WIDE), i32)),
        in_specs=[SM] + [VM] * 5,
        out_specs=(VM, VM, VM),
        scratch_shapes=[pltpu.VMEM((ex * grains + 8, LANES), f32)],
        compiler_params=pltpu.CompilerParams(vmem_limit_bytes=GRANT),
        cost_estimate=COST,
    )(lists, table, first, found, packed, named)

    margin, resid, loss_part = pl.pallas_call(
        functools.partial(residual_kernel, nf),
        out_shape=(shape((8, ex), f32), shape((1, ex), f32), shape((8, LANES), f32)),
        in_specs=[VM, VM],
        out_specs=(VM, VM, VM),
        scratch_shapes=[pltpu.VMEM((nf, 8, ex), f32), dma((nf - 1,)), dma((nf - 1,))],
        compiler_params=pltpu.CompilerParams(collective_id=1, has_side_effects=True, vmem_limit_bytes=GRANT),
        cost_estimate=COST,
    )(partial, labels.reshape(1, ex))

    rest = pl.pallas_call(
        functools.partial(late_kernel, grains, ready),
        out_shape=shape((deep * rows, 2 * width), f32),
        in_specs=[VM] * 4,
        out_specs=VM,
        scratch_shapes=[pltpu.SMEM((3 * hold, LANES), i32), pltpu.SMEM((1, ex), f32), dma((2,))],
        compiler_params=pltpu.CompilerParams(vmem_limit_bytes=GRANT),
        cost_estimate=COST,
    )(lists, resid, more_x2, more_high)

    total, notes = pl.pallas_call(
        functools.partial(scatter_kernel, n, grains),
        out_shape=(shape((rows, width), f32), shape((n, 8, LANES), f32)),
        in_specs=[VM] * 9,
        out_specs=(VM, VM),
        scratch_shapes=[
            pltpu.SMEM((3 * hold, LANES), i32),
            pltpu.SMEM((1, ex), f32),
            dma((2,)),
            pltpu.VMEM((n, 8, LANES), f32),
            pltpu.VMEM((steady + ready, 1, WIDE), f32),
            pltpu.VMEM((TOGETHER * rows, 2 * width), f32),
            pltpu.VMEM((deep, 2, rows, width), bf16),
            pltpu.VMEM((deep, rows, width), bf16),
            pltpu.VMEM((deep - 1, rows, width), bf16),
            pltpu.VMEM((deep, rows, width), bf16),
            dma((deep - 1,)),
            dma((deep,)),
            dma((deep,)),
            dma((deep,)),
            dma((n - 1,)),
            dma((n - 1,)),
        ],
        compiler_params=pltpu.CompilerParams(collective_id=2, has_side_effects=True, vmem_limit_bytes=GRANT),
        cost_estimate=COST,
    )(lists, rest, resid, x2, high, margin, owner, rank, loss_part)

    owned, gradient, loss = pl.pallas_call(
        finish_kernel,
        out_shape=(shape((1, ex), f32), shape((rows, width), f32), shape((1, 1), f32)),
        in_specs=[VM, VM],
        out_specs=(VM, VM, SM),
        compiler_params=pltpu.CompilerParams(vmem_limit_bytes=GRANT),
        cost_estimate=COST,
    )(total, notes)
    return owned.reshape(ex), gradient, loss.reshape(())


def solution(mesh):
    in_specs = (
        P("rows", "feat", None),
        P("rows", "feat"),
        P("rows", "feat"),
        P("rows"),
        P("rows"),
        P(("feat", "rows"), None),
    )
    out_specs = (P("rows"), P(("feat", "rows"), None), P())
    body = functools.partial(on_device, mesh.shape["rows"], mesh.shape["feat"])
    return jax.shard_map(body, mesh=mesh, in_specs=in_specs, out_specs=out_specs, check_vma=False)
```

```python
import functools

import jax
import jax.numpy as jnp
from jax import lax
from jax.experimental import pallas as pl
from jax.experimental.pallas import tpu as pltpu
from jax.sharding import PartitionSpec as P

MESH = pl.DeviceIdType.MESH
LANES = 128
GRAIN = 16
GROUP = 32
GRANT = 24 * 1024 * 1024
COST = pl.CostEstimate(flops=0, bytes_accessed=24 * 1024 * 1024, transcendentals=0)
NT = (((1,), (1,)), ((), ()))
NN = (((1,), (0,)), ((), ()))
VM = pl.BlockSpec(memory_space=pltpu.VMEM)
SM = pl.BlockSpec(memory_space=pltpu.SMEM)
ANY = pl.BlockSpec(memory_space=pltpu.HBM)
WIDE = GROUP * GRAIN
PER = LANES // GRAIN
CUT = 512
BATCH = 7
TOGETHER = 2


def seat(n):
    me = lax.axis_index("rows")
    side = lax.rem(me, 2)
    spot = me // 2
    partner = me + 1 - 2 * side
    deep = n // 2

    def listed(key):
        tables = [sorted((z for z in range(deep) if z != at), key=functools.partial(key, at)) for at in range(deep)]
        out = []
        for j in range(deep - 1):
            pick = tables[0][j]
            for at in range(1, deep):
                pick = pick + (tables[at][j] - tables[at - 1][j]) * ((spot + deep - at) // deep)
            out.append(pick)
        return out

    far = listed(lambda at, z: -abs(z - at))
    first = listed(lambda at, z: (abs(z - at)!=1, -abs(z - at)))
    return me, side, spot, partner, far, first


def call_out(axis, peers):
    barrier = pltpu.get_barrier_semaphore()
    for peer in peers:
        pl.semaphore_signal(barrier, inc=1, device_id={axis: peer}, device_id_type=MESH)
    return lambda: pl.semaphore_wait(barrier, len(peers))


def copy_to(axis, peer, source, target, send, recv):
    return pltpu.make_async_remote_copy(
        src_ref=source,
        dst_ref=target,
        send_sem=send,
        recv_sem=recv,
        device_id={axis: peer},
        device_id_type=MESH,
    )


def send_to(*args):
    copy = copy_to(*args)
    copy.start()
    return copy


def lane_group():
    return lax.broadcasted_iota(jnp.int32, (1, LANES), 1) // GRAIN


def own_lanes():
    sub = lax.broadcasted_iota(jnp.int32, (8, LANES), 0)
    return sub == lax.broadcasted_iota(jnp.int32, (8, LANES), 1) // GRAIN


def offsets(row):
    return jnp.broadcast_to(row, (8, WIDE)) - lax.broadcasted_iota(jnp.int32, (8, WIDE), 0)


def select_scores(pair, x2, offset, first, found):
    scores = lax.dot_general(pair, x2, NN, preferred_element_type=jnp.float32)
    for i in range(pair.shape[0] // 8):
        found = jnp.where(offset == first + i * 8, scores[i * 8 : i * 8 + 8, :], found)
    return found


def spread_sum(x2, offset, factor, firsts, rows):
    spread = jnp.concatenate(
        [jnp.where(offset == first + i * 8, factor, 0.0) for first in firsts for i in range(rows // 8)], axis=0
    ).astype(jnp.bfloat16)
    return lax.dot_general(spread, x2, NT, preferred_element_type=jnp.float32)


def put(x2_ref, hi_ref, t, values, id_row, rows):
    tall = x2_ref.shape[1] // 2
    chunk = id_row // rows
    odd = lax.rem(chunk, 2)
    hi_ref[t] = jnp.where(id_row < 0, -1, (chunk // 2) * rows + lax.rem(id_row, rows))
    odd = jnp.broadcast_to(odd.astype(jnp.float32), (16, WIDE))
    odd_half = jnp.concatenate([odd.astype(jnp.bfloat16)] * (tall // 16), axis=0)
    even_half = jnp.concatenate([(1.0 - odd).astype(jnp.bfloat16)] * (tall // 16), axis=0)
    flipped = values.T
    x2_ref[t, 0:tall, :] = flipped * even_half
    x2_ref[t, tall:, :] = flipped * odd_half


def listed_tiles(vals, idt, lists, t):
    hold = lists.shape[0] // 3
    row = t * GROUP // LANES
    col = lax.rem(t * GROUP, LANES)
    group = lane_group()
    values = jnp.concatenate([vals[lists[row, col + i]] for i in range(GROUP)], axis=0)
    parts = []
    for h in range(GROUP // PER):
        line = idt[pl.ds(lists[hold + row, col + h * PER], 1), :]
        for i in range(1, PER):
            line = jnp.where(group == i, idt[pl.ds(lists[hold + row, col + h * PER + i], 1), :], line)
        parts.append(line)
    return values, jnp.concatenate(parts, axis=1)


def gather_kernel(
    n, w_hbm, ids_hbm, used_hbm, owner_hbm, vals_hbm,
    table_ref, x2_ref, hi_ref, lists_ref, rank_ref, owner_ref, first_ref, rest_ref, vals, idt,
    w_buf, half, ids, used, own, lists, glist, found,
    send, recv, xsend, xrecv, here,
):
    local = [
        pltpu.make_async_copy(w_hbm, w_buf, here.at[0]),
        pltpu.make_async_copy(used_hbm, used, here.at[1]),
        pltpu.make_async_copy(ids_hbm, ids, here.at[2]),
        pltpu.make_async_copy(owner_hbm, own, here.at[3]),
        pltpu.make_async_copy(vals_hbm, vals, here.at[4]),
    ]
    for copy in local:
        copy.start()
    me, side, spot, partner, far, first = seat(n)
    deep = n // 2
    rows = w_buf.shape[0]
    slots, ex = ids.shape
    grains = slots // GRAIN
    joined = call_out("rows", [partner] + [2 * z + side for z in far])
    local[0].wait()
    half[...] = w_buf[...].astype(jnp.bfloat16)
    joined()
    across = [send_to("rows", partner, half, table_ref.at[me], xsend.at[spot], xrecv.at[spot])]
    along = [
        send_to("rows", 2 * z + side, half, table_ref.at[me], send.at[j], recv.at[spot])
        for j, z in enumerate(first)
    ]
    table_ref[me] = w_buf[...].astype(jnp.bfloat16)

    f32 = jnp.float32
    local[1].wait()
    count = (used[...] + (GRAIN - 1)) // GRAIN - 1
    sizes = jnp.broadcast_to(count, (LANES, ex)).T
    down = lax.broadcasted_iota(jnp.int32, (ex, LANES), 0)
    ends = sizes
    step = 1
    while step < ex:
        ends = ends + jnp.where(down >= step, pltpu.roll(ends, step, 0), 0)
        step *= 2
    lane = lax.broadcasted_iota(jnp.int32, (1, LANES), 1)
    span = ex * (grains - 1) // LANES
    hold = lists.shape[0] // 3
    for b in range(span):
        place = lane + b * LANES
        past = ends <= place
        which = jnp.sum(jnp.where(past, 1, 0), axis=0, keepdims=True)
        begin = jnp.sum(jnp.where(past, sizes, 0), axis=0, keepdims=True)
        live = which < ex
        q = place - begin + 1
        lists[b : b + 1, :] = jnp.clip(jnp.where(live, which * grains + q, 0), 0, grains * ex - 1)
        lists[hold + b : hold + b + 1, :] = jnp.clip(jnp.where(live, which + q * ex, grains * ex), 0, grains * ex)
    turns = (ends[ex - 8 : ex, :] + (GROUP - 1)) // GROUP
    lists[2 * hold :, :] = jnp.broadcast_to(turns[7:8, :], (hold, LANES))
    to_list = pltpu.make_async_copy(lists, glist, here.at[5])
    to_list.start()
    to_next = pltpu.make_async_copy(lists, lists_ref, here.at[6])
    to_next.start()

    local[2].wait()
    live = lax.broadcasted_iota(jnp.int32, (slots, ex), 0) < used[...]
    shifted = jnp.where(live, ids[...] + 1, 0)
    if slots < LANES:
        shifted = jnp.concatenate([shifted, jnp.zeros((LANES - slots, ex), jnp.int32)], axis=0)
    shifted = shifted.T
    grain_of = lax.broadcasted_iota(jnp.int32, (ex, LANES), 1) // GRAIN
    for q in range(grains):
        piece = jnp.where(grain_of == q, shifted, 0)
        step = GRAIN
        while step < LANES:
            piece = piece + pltpu.roll(piece, step, 1)
            step *= 2
        idt[q * ex : (q + 1) * ex, :] = piece - 1
    idt[grains * ex :, :] = jnp.full((8, LANES), -1, jnp.int32)

    mine = own_lanes()
    steady = ex // GROUP

    def prepare_first(t, carry):
        at = t * GROUP
        values = jnp.concatenate([vals[(at + i) * grains] for i in range(GROUP)], axis=0)
        parts = [
            jnp.sum(jnp.where(mine, idt[pl.ds(at + h * PER, PER), :], 0), axis=0, keepdims=True)
            for h in range(GROUP // PER)
        ]
        put(x2_ref, hi_ref, t, values, jnp.concatenate(parts, axis=1), rows)
        found[t] = jnp.zeros((8, WIDE), f32)
        return carry

    def prepare_rest(t, carry):
        values, id_row = listed_tiles(vals, idt, glist, t)
        put(x2_ref, hi_ref, steady + t, values, id_row, rows)
        found[steady + t] = jnp.zeros((8, WIDE), f32)
        return carry

    def score(z):
        pair = jnp.concatenate([table_ref[2 * z], table_ref[2 * z + 1]], axis=1)

        def turn(t, carry):
            found[t] = select_scores(pair, x2_ref[t], offsets(hi_ref[t]), z * rows, found[t])
            return carry

        lax.fori_loop(0, x2_ref.shape[0], turn, jnp.int32(0), unroll=True)

    local[4].wait()
    lax.fori_loop(0, steady, prepare_first, jnp.int32(0), unroll=2)
    to_list.wait()
    to_next.wait()

    def arrival(z):
        return copy_to("rows", partner, half, table_ref.at[2 * z + side], send.at[0], recv.at[z])

    def crossing(z):
        return copy_to("rows", partner, half, table_ref.at[2 * z + 1 - side], send.at[0], xrecv.at[z])

    local[3].wait()
    owner = own[...].astype(f32)
    square = jnp.broadcast_to(owner, (ex, ex))
    earlier = lax.broadcasted_iota(jnp.int32, (ex, ex), 0) < lax.broadcasted_iota(jnp.int32, (ex, ex), 1)
    same = jnp.where(jnp.logical_and(square.T == square, earlier), 1.0, 0.0)
    shift = lax.rem(me * (ex // n), LANES).astype(f32)
    rank = jnp.sum(same, axis=0, keepdims=True) + shift
    places = lax.broadcasted_iota(jnp.int32, (LANES, ex), 0).astype(f32)
    rank_ref[...] = jnp.where(places == rank, 1.0, 0.0)
    owner_ref[...] = jnp.broadcast_to(owner, owner_ref.shape)

    near = far[::-1]
    lax.fori_loop(0, x2_ref.shape[0] - steady, prepare_rest, jnp.int32(0), unroll=2)
    for j, z in enumerate(near):
        arrival(z).wait_recv()
        block = table_ref.at[2 * z + side]
        across.append(send_to("rows", partner, block, block, xsend.at[z], xrecv.at[z]))
        if j == 0:
            crossing(spot).wait_recv()
            score(spot)

    for z in near:
        crossing(z).wait_recv()
        score(z)
    for t in range(steady):
        term = jnp.sum(found[t], axis=0, keepdims=True)
        for h in range(GROUP // PER):
            at = t * GROUP + h * PER
            first_ref[at : at + PER, :] = jnp.where(mine, term[:, h * LANES : (h + 1) * LANES], 0.0)
    for t in range(x2_ref.shape[0] - steady):
        rest_ref[t] = jnp.sum(found[steady + t], axis=0, keepdims=True)
    for copy in along:
        copy.wait_send()
    for copy in across:
        copy.wait_send()


def margin_kernel(
    lists, table_ref, first_ref, rest_ref, vals, idt, partial_ref, more_x2, more_hi, terms
):
    n, rows, _ = table_ref.shape
    ex = partial_ref.shape[1]
    grains = terms.shape[0] // ex
    hold = lists.shape[0] // 3
    ready = rest_ref.shape[0]
    terms[ex:, :] = jnp.zeros((terms.shape[0] - ex, LANES), jnp.float32)
    group = lane_group()

    def one(x2, row):
        offset = offsets(row)
        found = jnp.zeros((8, WIDE), jnp.float32)
        for k in range(n // 2):
            pair = jnp.concatenate([table_ref[2 * k], table_ref[2 * k + 1]], axis=1)
            found = select_scores(pair, x2, offset, k * rows, found)
        return jnp.sum(found, axis=0, keepdims=True)

    def keep(t, term):
        row = t * GROUP // LANES
        col = lax.rem(t * GROUP, LANES)
        for i in range(GROUP):
            h = i // PER
            mine = jnp.where(group == i % PER, term[:, h * LANES : (h + 1) * LANES], 0.0)
            terms[pl.ds(lists[hold + row, col + i], 1), :] = mine

    def turn(t, carry):
        keep(t, rest_ref[t])
        return carry

    def late_turn(t, carry):
        values, id_row = listed_tiles(vals, idt, lists, t)
        put(more_x2, more_hi, t - ready, values, id_row, rows)
        keep(t, one(more_x2[t - ready], more_hi[t - ready]))
        return carry

    turns = lists[2 * hold, 0]
    lax.fori_loop(0, jnp.minimum(turns, ready), turn, jnp.int32(0))
    lax.fori_loop(ready, turns, late_turn, jnp.int32(0))
    spread = first_ref[...]
    for q in range(1, grains):
        spread = spread + terms[q * ex : (q + 1) * ex, :]
    partial_ref[...] = jnp.broadcast_to(jnp.sum(spread.T, axis=0, keepdims=True), partial_ref.shape)


def residual_kernel(n, partial_ref, labels_ref, margin_ref, resid_ref, loss_ref, held, send, recv):
    me = lax.axis_index("feat")
    peers = [lax.rem(me + k, n) for k in range(1, n)]
    call_out("feat", peers)()
    copies = [
        send_to("feat", peer, partial_ref, held.at[me], send.at[k], recv.at[k])
        for k, peer in enumerate(peers)
    ]
    held[me] = partial_ref[...]
    for copy in copies:
        copy.wait()
    margin = held[0]
    for k in range(1, n):
        margin = margin + held[k]
    label = labels_ref[...].astype(jnp.float32)
    residual = 1.0 / (1.0 + jnp.exp(-margin)) - label
    margin_ref[...] = margin
    resid_ref[...] = residual.astype(jnp.bfloat16).astype(jnp.float32)[0:1, :]
    term = jnp.maximum(margin, 0.0) + jnp.log1p(jnp.exp(-jnp.abs(margin))) - label * margin
    total = term[:, 0:LANES]
    for h in range(1, term.shape[1] // LANES):
        total = total + term[:, h * LANES : (h + 1) * LANES]
    loss_ref[...] = total


def factor_row(grains, lists, resid, t):
    group = lane_group()
    row_at = t * GROUP // LANES
    col = lax.rem(t * GROUP, LANES)
    parts = []
    for h in range(GROUP // PER):
        row = jnp.zeros((1, LANES), jnp.float32)
        for i in range(PER):
            row = jnp.where(group == i, resid[0, lists[row_at, col + h * PER + i] // grains], row)
        parts.append(row)
    return jnp.concatenate(parts, axis=1)


def late_kernel(grains, ready, lists_ref, resid_ref, more_x2, more_hi, total, lists, resid, here):
    hold = lists.shape[0] // 3

    def turn(t, carry):
        factor = jnp.broadcast_to(factor_row(grains, lists, resid, t), (8, WIDE))
        x2, offset = more_x2[t - ready], offsets(more_hi[t - ready])
        for k in range(0, total.shape[0], CUT):
            total[k : k + CUT, :] += spread_sum(x2, offset, factor, [k], CUT)
        return carry

    @pl.when(jnp.max(lists_ref[2 * hold :, :]) > ready)
    def _():
        copies = [
            pltpu.make_async_copy(lists_ref, lists, here.at[0]),
            pltpu.make_async_copy(resid_ref, resid, here.at[1]),
        ]
        for copy in copies:
            copy.start()
        total[...] = jnp.zeros_like(total)
        for copy in copies:
            copy.wait()
        lax.fori_loop(ready, lists[2 * hold, 0], turn, jnp.int32(0))


def scatter_kernel(
    n, grains, lists_ref, rest_ref, resid_ref, x2_ref, hi_ref, margin_ref, owner_ref, rank_ref, loss_ref,
    sum_ref, notes_ref,
    lists, resid, here, notes, factors, acc, part, crossed, paired, held, send, recv, xsend, xrecv, nsend, nrecv,
):
    ex = margin_ref.shape[1]
    me, side, spot, partner, far, first = seat(n)
    deep = n // 2
    rows, width = sum_ref.shape
    others = [lax.rem(me + k, n) for k in range(1, n)]
    joined = call_out("rows", others)
    local = [
        pltpu.make_async_copy(lists_ref, lists, here.at[0]),
        pltpu.make_async_copy(resid_ref, resid, here.at[1]),
    ]
    for copy in local:
        copy.start()
    mine = own_lanes()
    steady = ex // GROUP
    ready = x2_ref.shape[0] - steady
    hold = lists.shape[0] // 3
    tall = jnp.broadcast_to(resid_ref[...], (LANES, ex)).T
    for t in range(steady):
        parts = [
            jnp.sum(
                jnp.where(mine, tall[t * GROUP + h * PER : t * GROUP + (h + 1) * PER, :], 0.0), axis=0, keepdims=True
            )
            for h in range(GROUP // PER)
        ]
        factors[t] = jnp.concatenate(parts, axis=1)
    for copy in local:
        copy.wait()

    def listed_factor(t, carry):
        factors[steady + t] = factor_row(grains, lists, resid, t)
        return carry

    lax.fori_loop(0, ready, listed_factor, jnp.int32(0), unroll=2)
    late = jnp.broadcast_to(lists_ref[2 * hold : 2 * hold + 1, 0:1] > ready, (rows, 2 * width))

    batch = max(b for b in range(1, BATCH + 1) if (steady + ready) % b == 0)

    def gather_pairs(js, zs):
        for i, z in enumerate(zs):
            more = rest_ref[pl.ds(pl.multiple_of(z * rows, rows), rows), :]
            acc[i * rows : (i + 1) * rows, :] = jnp.where(late, more, 0.0)
        high = len(js) * rows

        def turn(step, carry):
            part_sum = None
            for i in range(batch):
                t = step * batch + i
                factor = jnp.broadcast_to(factors[t], (8, WIDE))
                more = spread_sum(x2_ref[t], offsets(hi_ref[t]), factor, [z * rows for z in zs], rows)
                part_sum = more if part_sum is None else part_sum + more
            acc[0:high, :] += part_sum
            return carry

        lax.fori_loop(0, (steady + ready) // batch, turn, jnp.int32(0))
        for i, j in enumerate(js):
            part[j, 0] = acc[i * rows : (i + 1) * rows, 0:width].astype(jnp.bfloat16)
            part[j, 1] = acc[i * rows : (i + 1) * rows, width:].astype(jnp.bfloat16)

    def cross(j):
        return send_to("rows", partner, part.at[j, 1 - side], crossed.at[j], xsend.at[j], xrecv.at[j])

    across = []
    along = []

    def pass_on(j):
        across[j].wait_recv()
        pair = part[j, side].astype(jnp.float32) + crossed[j].astype(jnp.float32)
        paired[j] = pair.astype(jnp.bfloat16)
        along.append(
            send_to("rows", 2 * far[j] + side, paired.at[j], held.at[spot], send.at[j], recv.at[spot])
        )

    last = deep - 1
    planes = far + [spot]
    for j in range(0, deep, TOGETHER):
        js = list(range(j, min(j + TOGETHER, deep)))
        gather_pairs(js, [planes[i] for i in js])
        if j == 0:
            joined()
        across += [cross(i) for i in js]

    which = lax.broadcasted_iota(jnp.int32, (n, ex), 0).astype(jnp.float32)
    by_owner = jnp.where(which == owner_ref[0:1, :], margin_ref[0:1, :], 0.0)
    ordered = lax.dot_general(
        by_owner, rank_ref[...], NT, precision=lax.Precision.HIGHEST, preferred_element_type=jnp.float32
    )
    sub = lax.broadcasted_iota(jnp.int32, (8, LANES), 0)
    for d in range(n):
        notes[d] = jnp.where(sub == 0, ordered[d : d + 1, :], loss_ref[...])
    told = [
        send_to("rows", peer, notes.at[peer], notes_ref.at[me], nsend.at[k], nrecv.at[k])
        for k, peer in enumerate(others)
    ]
    notes_ref[me] = notes[me]
    for j in range(last):
        pass_on(j)
    across[last].wait_recv()
    total = part[last, side].astype(jnp.float32) + crossed[last].astype(jnp.float32)
    for z in far[::-1]:
        copy_to("rows", partner, paired.at[0], held.at[z], send.at[0], recv.at[z]).wait_recv()
        total = total + held[z].astype(jnp.float32)
    sum_ref[...] = total
    for copy in across:
        copy.wait_send()
    for copy in along:
        copy.wait_send()
    for copy in told:
        copy.wait()


def finish_kernel(sum_ref, notes_ref, owned_ref, grad_ref, loss_ref):
    n = notes_ref.shape[0]
    ex = owned_ref.shape[1]
    grad_ref[...] = sum_ref[...]
    for h in range(ex // LANES):
        row = jnp.zeros((1, LANES), jnp.float32)
        for d in range(n):
            if d * (ex // n) // LANES == h:
                row = row + notes_ref[d, 0:1, :]
        owned_ref[:, h * LANES : (h + 1) * LANES] = row
    loss = jnp.zeros((1, LANES), jnp.float32)
    for d in range(n):
        loss = loss + notes_ref[d, 1:2, :]
    loss_ref[0, 0] = jnp.sum(loss) * (1.0 / (ex * n))


def on_device(n, nf, tile_values, tile_blocks, tile_counts, labels, owner_rank, weights):
    ex, slots, width = tile_values.shape
    grains = slots // GRAIN
    rows = weights.shape[0]
    deep = n // 2
    steady = ex // GROUP
    ready = min(6, (grains - 1) * steady)
    late = max((grains - 1) * steady - ready, 1)
    hold = -(-(ex * (grains - 1)) // (8 * LANES)) * 8
    f32, i32, bf16 = jnp.float32, jnp.int32, jnp.bfloat16
    shape = jax.ShapeDtypeStruct
    dma = pltpu.SemaphoreType.DMA
    vals = tile_values.reshape(ex * grains, GRAIN, width)

    table, x2, high, lists, rank, owner, first, found, packed, named = pl.pallas_call(
        functools.partial(gather_kernel, n),
        out_shape=(
            shape((n, rows, width), bf16),
            shape((steady + ready, 2 * width, WIDE), bf16),
            shape((steady + ready, 1, WIDE), i32),
            shape((3 * hold, LANES), i32),
            shape((LANES, ex), f32),
            shape((8, ex), f32),
            shape((ex, LANES), f32),
            shape((ready, 1, WIDE), f32),
            shape((ex * grains, GRAIN, width), bf16),
            shape((ex * grains + 8, LANES), i32),
        ),
        in_specs=[ANY] * 5,
        out_specs=(VM, VM, VM, SM, VM, VM, VM, VM, VM, VM),
        scratch_shapes=[
            pltpu.VMEM((rows, width), f32),
            pltpu.VMEM((rows, width), bf16),
            pltpu.VMEM((slots, ex), i32),
            pltpu.VMEM((1, ex), i32),
            pltpu.VMEM((1, ex), i32),
            pltpu.VMEM((3 * hold, LANES), i32),
            pltpu.SMEM((3 * hold, LANES), i32),
            pltpu.VMEM((steady + ready, 8, WIDE), f32),
            dma((deep - 1,)), dma((deep,)), dma((deep,)), dma((deep,)), dma((7,)),
        ],
        compiler_params=pltpu.CompilerParams(collective_id=0, has_side_effects=True, vmem_limit_bytes=GRANT),
        cost_estimate=COST,
    )(*[
        pltpu.with_memory_space_constraint(a, pltpu.HBM)
        for a in (weights, tile_blocks.T, tile_counts.reshape(1, ex), owner_rank.reshape(1, ex), vals)
    ])

    partial, more_x2, more_high = pl.pallas_call(
        margin_kernel,
        out_shape=(shape((8, ex), f32), shape((late, 2 * width, WIDE), bf16), shape((late, 1, WIDE), i32)),
        in_specs=[SM] + [VM] * 5,
        out_specs=(VM, VM, VM),
        scratch_shapes=[pltpu.VMEM((ex * grains + 8, LANES), f32)],
        compiler_params=pltpu.CompilerParams(vmem_limit_bytes=GRANT),
        cost_estimate=COST,
    )(lists, table, first, found, packed, named)

    margin, resid, loss_part = pl.pallas_call(
        functools.partial(residual_kernel, nf),
        out_shape=(shape((8, ex), f32), shape((1, ex), f32), shape((8, LANES), f32)),
        in_specs=[VM, VM],
        out_specs=(VM, VM, VM),
        scratch_shapes=[pltpu.VMEM((nf, 8, ex), f32), dma((nf - 1,)), dma((nf - 1,))],
        compiler_params=pltpu.CompilerParams(collective_id=1, has_side_effects=True, vmem_limit_bytes=GRANT),
        cost_estimate=COST,
    )(partial, labels.reshape(1, ex))

    rest = pl.pallas_call(
        functools.partial(late_kernel, grains, ready),
        out_shape=shape((deep * rows, 2 * width), f32),
        in_specs=[VM] * 4,
        out_specs=VM,
        scratch_shapes=[pltpu.SMEM((3 * hold, LANES), i32), pltpu.SMEM((1, ex), f32), dma((2,))],
        compiler_params=pltpu.CompilerParams(vmem_limit_bytes=GRANT),
        cost_estimate=COST,
    )(lists, resid, more_x2, more_high)

    total, notes = pl.pallas_call(
        functools.partial(scatter_kernel, n, grains),
        out_shape=(shape((rows, width), f32), shape((n, 8, LANES), f32)),
        in_specs=[VM] * 9,
        out_specs=(VM, VM),
        scratch_shapes=[
            pltpu.SMEM((3 * hold, LANES), i32),
            pltpu.SMEM((1, ex), f32),
            dma((2,)),
            pltpu.VMEM((n, 8, LANES), f32),
            pltpu.VMEM((steady + ready, 1, WIDE), f32),
            pltpu.VMEM((TOGETHER * rows, 2 * width), f32),
            pltpu.VMEM((deep, 2, rows, width), bf16),
            pltpu.VMEM((deep, rows, width), bf16),
            pltpu.VMEM((deep - 1, rows, width), bf16),
            pltpu.VMEM((deep, rows, width), bf16),
            dma((deep - 1,)),
            dma((deep,)),
            dma((deep,)),
            dma((deep,)),
            dma((n - 1,)),
            dma((n - 1,)),
        ],
        compiler_params=pltpu.CompilerParams(collective_id=2, has_side_effects=True, vmem_limit_bytes=GRANT),
        cost_estimate=COST,
    )(lists, rest, resid, x2, high, margin, owner, rank, loss_part)

    owned, gradient, loss = pl.pallas_call(
        finish_kernel,
        out_shape=(shape((1, ex), f32), shape((rows, width), f32), shape((1, 1), f32)),
        in_specs=[VM, VM],
        out_specs=(VM, VM, SM),
        compiler_params=pltpu.CompilerParams(vmem_limit_bytes=GRANT),
        cost_estimate=COST,
    )(total, notes)
    return owned.reshape(ex), gradient, loss.reshape(())


def solution(mesh):
    in_specs = (
        P("rows", "feat", None),
        P("rows", "feat"),
        P("rows", "feat"),
        P("rows"),
        P("rows"),
        P(("feat", "rows"), None),
    )
    out_specs = (P("rows"), P(("feat", "rows"), None), P())
    body = functools.partial(on_device, mesh.shape["rows"], mesh.shape["feat"])
    return jax.shard_map(body, mesh=mesh, in_specs=in_specs, out_specs=out_specs, check_vma=False)
```
